128 devices in a mesh: row: 8 (over y, core), col: 16 (over x, z).
Axes of the slice: x: 4, y: 4, z: 4, core: 2. Of those that a mesh axis runs over, the one named last changes fastest.
Arguments:
- coupling_panel: bfloat16 [8, 1536, 512], P('row'), may hold values from -6 to 6
- interior_factor: float32 [8, 1536, 1536], P('row'), may hold values from -1 to 3, as said below
- border_rows: bfloat16 [8, 8192, 1536], P('row', 'col'), may hold values from -0.109375 to 0.109375
- target_rows: int32 [8, 8192], P('row', 'col'), may hold values from 0 to 32767, as said below
- border_block: float32 [32768, 512], P(('row', 'col')), may hold values from -6 to 6
Outputs:
- schur_panel: float32 [32768, 512], P(('row', 'col'))
The draws below stay inside these ranges and needn't reach their ends.
Inputs may be any that keep to these rules, and one draw needn't show every extreme that they name: `target_rows`: each block of 512 entries along the second dimension (the rows of one device) is nondecreasing. Row g of the Schur panel is held by device g // 256 in the order of row+col. The rows of one device name any one holder at most 8 times, and some holder is named exactly 8 times by the rows of every device. `interior_factor`: each [1536, 1536] block is lower triangular with diagonal entries between 1 and 3.
All inputs are finite; a program needn't handle non-finite values.
Results may differ from the reference program's by a relative error of at most 0.0029.
Values may be sent and summed in bfloat16 or wider, within the bound.
A program may use at most 128 MiB of HBM per device.

```python
import jax
import jax.numpy as jnp
from jax import lax

PANEL = 512
INTERIOR = 1536
BORDER_DEV = 512
OWNED_DEV = 256
NI = 32768
DEPTH = 8
SUBTREES = 8
N_ROW = 8
N_COL = 16
DEVICES = 128


def draw_interior_factor(key, part):
    diag_key, lower_key = jax.random.split(key)
    diagonal = jax.random.uniform(diag_key, (SUBTREES, INTERIOR), jnp.float32, 1.0, 2.0)
    off_scale = 2.7
    lower_part = jax.random.normal(lower_key, (SUBTREES, INTERIOR, INTERIOR), jnp.float32)
    lower_part = jnp.clip(jnp.clip(lower_part, -4.0, 4.0) * (off_scale / INTERIOR ** 0.5), -1.0, 1.0)
    strict = jnp.tril(jnp.ones((INTERIOR, INTERIOR), jnp.float32), -1)
    identity = jnp.eye(INTERIOR, dtype=jnp.float32)
    return lower_part * strict[None] + diagonal[:, :, None] * identity[None]


def draw_target_rows(key, part):
    hottest = jax.random.randint(jax.random.fold_in(key, 11), (), 0, DEVICES)
    tiers = jax.random.randint(jax.random.fold_in(key, 12), (DEVICES,), 0, 4)
    others = jnp.arange(DEVICES - 1, dtype=jnp.int32)
    other_owner = others + (others >= hottest).astype(jnp.int32)
    candidates = jnp.arange((DEVICES - 1) * DEPTH, dtype=jnp.int32)
    cand_owner = other_owner[candidates // DEPTH]

    def one_source(source):
        source_key = jax.random.fold_in(key, 100 + source)
        noise = jax.random.randint(source_key, candidates.shape, 0, 16384)
        scores = (tiers[cand_owner] * 4096 + noise) * 8192 + candidates
        unused, chosen = lax.top_k(scores, BORDER_DEV - DEPTH)
        holders = jnp.concatenate([jnp.full((DEPTH,), hottest, jnp.int32), cand_owner[chosen]])
        within = jax.random.randint(jax.random.fold_in(source_key, 7), (BORDER_DEV,), 0, OWNED_DEV)
        return jnp.sort(holders * OWNED_DEV + within)
    flat = jax.vmap(one_source)(jnp.arange(DEVICES, dtype=jnp.int32))
    return flat.reshape(N_ROW, N_COL * BORDER_DEV).astype(jnp.int32)


def block_levels(stream_key, dims, shards, least, largest):
    level = 1.0
    for dim, blocks in shards:
        draws = jax.random.uniform(jax.random.fold_in(jax.random.fold_in(stream_key, 6), dim), (blocks,), jnp.float32, least / len(shards), largest / len(shards))
        level = level * jnp.repeat(jnp.exp(draws), dims[dim] // blocks).reshape((-1,) + (1,) * (len(dims) - 1 - dim))
    return level


def scatter_about(rng, extent, width, limit, cuts=(), kind=jnp.bfloat16):
    result = width * jax.random.normal(rng, extent, jnp.float32)
    if cuts:
        result = result * block_levels(rng, extent, cuts, -0.22, 0.18)
    return jnp.clip(result, -limit, limit).astype(kind)


def setup_inputs(seed: int = 0) -> dict:
    key_of = jax.random.split(jax.random.key(seed), 6)
    return {
        "coupling_panel": scatter_about(key_of[0], (SUBTREES, INTERIOR, PANEL), 1.0, 6.0, ((0, 8),)),
        "interior_factor": draw_interior_factor(jax.random.fold_in(key_of[5], 71), 0),
        "border_rows": scatter_about(key_of[2], (SUBTREES, N_COL * BORDER_DEV, INTERIOR), (2 * INTERIOR) ** -0.5, 0.109375, ((0, 8), (1, 16))),
        "target_rows": draw_target_rows(jax.random.fold_in(key_of[5], 71), 0),
        "border_block": scatter_about(key_of[4], (NI, PANEL), 1.0, 6.0, ((0, 128),), jnp.float32),
    }


def substitute(factor, panel_cols):
    forward = lax.linalg.triangular_solve(factor, panel_cols, left_side=True, lower=True)
    return lax.linalg.triangular_solve(factor, forward, left_side=True, lower=True, transpose_a=True)

def reference(coupling_panel, interior_factor, border_rows, target_rows, border_block):

    def subtree(assembled, pieces):
        panel_cols, factor, coupling_rows, targets = pieces
        solved = substitute(factor, panel_cols.astype(jnp.float32)).astype(jnp.bfloat16)
        update = jnp.dot(coupling_rows.astype(jnp.float32), solved.astype(jnp.float32), preferred_element_type=jnp.float32)
        return (assembled.at[targets.astype(jnp.int32)].add(update), None)
    initial = jnp.zeros(border_block.shape, jnp.float32)
    assembled, unused = lax.scan(subtree, initial, (coupling_panel, interior_factor, border_rows, target_rows))
    return border_block - assembled
```

```python
import jax
import jax.numpy as jnp
from jax import lax
from jax.experimental import pallas as pl
from jax.experimental.pallas import tpu as pltpu
from jax.sharding import PartitionSpec as P

F32, BF16, I32 = jnp.float32, jnp.bfloat16, jnp.int32
BASE = 32
TILE = 256
BIG = 512
CHUNK = 256
SLOTS = 8
LOGICAL = pl.DeviceIdType.LOGICAL
EMPTY = -512.0


def iota(shape, axis):
    return lax.broadcasted_iota(I32, shape, axis)


def split(x):
    hi = x.astype(BF16)
    return hi, (x - hi.astype(F32)).astype(BF16)


def mm(a, b):
    return jnp.dot(a, b, preferred_element_type=F32)


def mm_nt(a, b):
    return lax.dot_general(a, b, (((1,), (1,)), ((), ())), preferred_element_type=F32)


def mm3(a, b):
    return mm(a[0], b[0]) + (mm(a[0], b[1]) + mm(a[1], b[0]))


def invert_base(strip):
    rows, width = strip.shape
    lane = iota((rows, width), 1)
    row = iota((rows, width), 0)
    within = lane % BASE
    start = lane - within
    tiles = range(0, width, 128)
    local = (lane - within)[:, :128] % 128

    def pick(x, index):
        return jnp.concatenate(
            [jnp.take_along_axis(x[:, t : t + 128], index[: x.shape[0]], axis=1) for t in tiles], axis=1
        )

    recip = 1.0 / pick(strip, local + row[:, :128])
    scaled = jnp.where(within < row, strip * recip, 0.0)
    inverse = jnp.where(within == row, recip, 0.0)
    for k in range(rows - 1):
        first = (k + 1) // 8 * 8
        factor = pick(scaled[first:], local + k)
        update = inverse[first:] - factor * inverse[k : k + 1]
        inverse = update if first == 0 else jnp.concatenate([inverse[:first], update], axis=0)
    return inverse


def merge_mask(size):
    r, c = iota((TILE, TILE), 0), iota((TILE, TILE), 1)
    return (r // (2 * size) == c // (2 * size)) & (r // size % 2 == 1) & (c // size % 2 == 0)


def kernel(
    panel_ref, factor_ref, rows_ref, target_ref, block_ref, out_ref,
    diag, sub, off, vh, vl, oh, ol, fwd, sol, place, send, recv, send_idx, recv_idx,
    load_sem, send_sem, recv_sem,
):
    n_holders = lax.axis_size("row") * lax.axis_size("col")
    me = lax.axis_index("row") * lax.axis_size("col") + lax.axis_index("col")
    n_big = off.shape[0]
    n_tile = diag.shape[0]
    pairs = [(1, 0), (2, 0), (2, 1)]

    loads = []

    def load(src_rows, src_cols, dst, sem):
        cp = pltpu.make_async_copy(factor_ref.at[src_rows, src_cols], dst, sem)
        cp.start()
        return cp

    load_diag = [
        load(pl.ds(t * TILE, TILE), pl.ds(t * TILE, TILE), diag.at[t], load_sem.at[t]) for t in range(n_tile)
    ]
    load_sub = [
        load(pl.ds((2 * t + 1) * TILE, TILE), pl.ds(2 * t * TILE, TILE), sub.at[t], load_sem.at[n_tile + t])
        for t in range(n_big)
    ]
    load_off = [
        load(pl.ds(i * BIG, BIG), pl.ds(j * BIG, BIG), off.at[p], load_sem.at[n_tile + n_big + p])
        for p, (i, j) in enumerate(pairs)
    ]

    barrier = pltpu.get_barrier_semaphore()

    def greet(o, carry):
        pl.semaphore_signal(barrier, inc=1, device_id=lax.rem(me + o, n_holders), device_id_type=LOGICAL)
        return carry

    lax.fori_loop(1, n_holders, greet, 0)

    sent = target_ref.shape[1]
    target = jnp.broadcast_to(target_ref[...], (8, sent))
    holder = target // block_ref.shape[0]
    within = target - holder * block_ref.shape[0]
    lane = iota((8, sent), 1)
    rank = jnp.zeros((8, sent), I32)
    for d in range(1, SLOTS):
        same = (pltpu.roll(holder, d, 1) == holder) & (lane >= d)
        rank = rank + jnp.where(same, 1, 0)
    position = (holder * SLOTS + rank)[:1]
    slots = n_holders * SLOTS
    placed = jnp.where(iota((slots, sent), 0) == position, 1.0, 0.0).astype(BF16)
    place[...] = placed
    described = jnp.concatenate(
        [jnp.broadcast_to(within[:1].astype(F32), (128, sent)), jnp.ones((128, sent), F32)], axis=0
    ).astype(BF16)
    found = mm_nt(placed, described)
    index = (found[:, :128] + EMPTY * (1.0 - found[:, 128:])).reshape(n_holders, SLOTS, 128)
    send_idx[...] = jnp.concatenate([index, index], axis=1).astype(BF16)

    for cp in load_diag:
        cp.wait()
    parts = []
    group = iota((BASE, 128), 1) // BASE
    for t in range(n_tile):
        for half in range(2):
            lo = half * 128
            tile = diag[t, lo : lo + 128, lo : lo + 128]
            strip = tile[:BASE]
            for q in range(1, 128 // BASE):
                strip = jnp.where(group == q, tile[q * BASE : (q + 1) * BASE], strip)
            parts.append(strip)
    base = invert_base(jnp.concatenate(parts, axis=1))
    wide = iota((BASE, TILE), 1) // BASE
    inverse = []
    for t in range(n_tile):
        piece = base[:, t * TILE : (t + 1) * TILE]
        inverse.append(
            jnp.concatenate([jnp.where(wide == q, piece, 0.0) for q in range(TILE // BASE)], axis=0)
        )
    size = BASE
    while size < TILE:
        mask = merge_mask(size)
        for t in range(n_tile):
            v = split(inverse[t])
            low = split(jnp.where(mask, diag[t], 0.0))
            inverse[t] = inverse[t] - mm3(v, split(mm3(low, v)))
        size *= 2
    for cp in load_sub:
        cp.wait()
    for b in range(n_big):
        top, bottom = split(inverse[2 * b]), split(inverse[2 * b + 1])
        left = split(mm3(bottom, split(mm3(split(sub[b]), top))))
        for ref, i, sign in ((vh, 0, 1), (vl, 1, 1)):
            ref[b, :TILE, :TILE] = top[i]
            ref[b, TILE:, TILE:] = bottom[i]
            ref[b, TILE:, :TILE] = -left[i]

    for p in range(len(pairs)):
        load_off[p].wait()
        oh[p], ol[p] = split(off[p])

    pl.semaphore_wait(barrier, n_holders - 1)

    def dispatch(source, target_buf, sem_at):
        def one(o, carry):
            to = lax.rem(me + o, n_holders)
            pltpu.make_async_remote_copy(
                src_ref=source.at[to],
                dst_ref=target_buf.at[me],
                send_sem=send_sem.at[sem_at],
                recv_sem=recv_sem.at[sem_at],
                device_id=to,
                device_id_type=LOGICAL,
            ).start()
            return carry

        lax.fori_loop(1, n_holders, one, 0)
        target_buf[me] = source[me]

    def arrived(source, target_buf, sem_at):
        others = pl.ds(0, n_holders - 1)
        pltpu.make_async_copy(source.at[others], target_buf.at[others], recv_sem.at[sem_at]).wait()

    def left_device(source, target_buf, sem_at):
        others = pl.ds(0, n_holders - 1)
        pltpu.make_async_copy(source.at[others], target_buf.at[others], send_sem.at[sem_at]).wait()

    dispatch(send_idx, recv_idx, 0)

    def block_inv(b):
        return (vh[b], vl[b])

    n_chunk = send.shape[0]
    for ch in range(n_chunk):
        cols = slice(ch * CHUNK, (ch + 1) * CHUNK)
        rhs = [panel_ref[b * BIG : (b + 1) * BIG, cols].astype(F32) for b in range(n_big)]
        for b in range(n_big):
            r = split(rhs[b])
            v = block_inv(b)
            upper = mm3((v[0][:TILE, :TILE], v[1][:TILE, :TILE]), (r[0][:TILE], r[1][:TILE]))
            lower = mm3((v[0][TILE:], v[1][TILE:]), r)
            f = jnp.concatenate([upper, lower], axis=0)
            fwd[:, b * BIG : (b + 1) * BIG] = f.T
            fs = split(f)
            for p, (i, j) in enumerate(pairs):
                if j == b:
                    rhs[i] = rhs[i] - mm3((oh[p], ol[p]), fs)
        for b in reversed(range(n_big)):
            q = split(fwd[:, b * BIG : (b + 1) * BIG])
            v = block_inv(b)
            first = mm3(q, (v[0][:, :TILE], v[1][:, :TILE]))
            second = mm3((q[0][:, TILE:], q[1][:, TILE:]), (v[0][TILE:, TILE:], v[1][TILE:, TILE:]))
            x = jnp.concatenate([first, second], axis=1)
            xs = split(x)
            sol[:, b * BIG : (b + 1) * BIG] = xs[0]
            for p, (i, j) in enumerate(pairs):
                if i == b:
                    at = slice(j * BIG, (j + 1) * BIG)
                    fwd[:, at] = fwd[:, at] - mm3(xs, (oh[p], ol[p]))
        update = mm_nt(rows_ref[...], sol[...]).astype(BF16)
        packed = mm(place[...], update).reshape(n_holders, SLOTS, CHUNK)
        send[ch] = jnp.concatenate([packed[:, :, :128], packed[:, :, 128:]], axis=1).astype(BF16)
        dispatch(send.at[ch], recv.at[ch], 1 + ch)

    arrived(send_idx, recv_idx, 0)
    owned = block_ref.shape[0]
    pick0 = jnp.where(iota((8, 128), 1) == 0, 1.0, 0.0).astype(BF16)
    named = mm_nt(pick0, recv_idx[...].reshape(n_holders * 2 * SLOTS, 128))[:1]
    total = n_holders * 2 * SLOTS
    named = named + jnp.where(iota((1, total), 1) // SLOTS % 2 == 1, float(owned), 0.0)
    gather = jnp.where(iota((2 * owned, total), 0).astype(F32) == named, 1.0, 0.0).astype(BF16)
    for ch in range(n_chunk):
        arrived(send.at[ch], recv.at[ch], 1 + ch)
        summed = mm(gather, recv[ch].reshape(total, 128))
        for half in range(2):
            cols = slice(ch * CHUNK + half * 128, ch * CHUNK + (half + 1) * 128)
            out_ref[:, cols] = block_ref[:, cols] - summed[half * owned : (half + 1) * owned]
    left_device(send_idx, recv_idx, 0)
    for ch in range(n_chunk):
        left_device(send.at[ch], recv.at[ch], 1 + ch)


def local(coupling_panel, interior_factor, border_rows, target_rows, border_block):
    panel, factor, rows = coupling_panel[0], interior_factor[0], border_rows[0]
    n, width = panel.shape
    holders = lax.axis_size("row") * lax.axis_size("col")
    n_tile, n_big, n_chunk = n // TILE, n // BIG, width // CHUNK
    pairs = n_big * (n_big - 1) // 2
    vmem = pl.BlockSpec(memory_space=pltpu.VMEM)
    return pl.pallas_call(
        kernel,
        out_shape=jax.ShapeDtypeStruct(border_block.shape, F32),
        in_specs=[vmem, pl.BlockSpec(memory_space=pl.ANY), vmem, vmem, vmem],
        out_specs=vmem,
        scratch_shapes=[
            pltpu.VMEM((n_tile, TILE, TILE), F32),
            pltpu.VMEM((n_big, TILE, TILE), F32),
            pltpu.VMEM((pairs, BIG, BIG), F32),
            pltpu.VMEM((n_big, BIG, BIG), BF16),
            pltpu.VMEM((n_big, BIG, BIG), BF16),
            pltpu.VMEM((pairs, BIG, BIG), BF16),
            pltpu.VMEM((pairs, BIG, BIG), BF16),
            pltpu.VMEM((CHUNK, n), F32),
            pltpu.VMEM((CHUNK, n), BF16),
            pltpu.VMEM((holders * SLOTS, target_rows.shape[1]), BF16),
            pltpu.VMEM((n_chunk, holders, 2 * SLOTS, 128), BF16),
            pltpu.VMEM((n_chunk, holders, 2 * SLOTS, 128), BF16),
            pltpu.VMEM((holders, 2 * SLOTS, 128), BF16),
            pltpu.VMEM((holders, 2 * SLOTS, 128), BF16),
            pltpu.SemaphoreType.DMA((n_tile + n_big + pairs,)),
            pltpu.SemaphoreType.DMA((1 + n_chunk,)),
            pltpu.SemaphoreType.DMA((1 + n_chunk,)),
        ],
        compiler_params=pltpu.CompilerParams(
            collective_id=0, has_side_effects=True, vmem_limit_bytes=60 * 1024 * 1024
        ),
        name="schur_panel",
    )(panel, factor, rows, target_rows, border_block)


def solution(mesh):
    placed = (
        P("row", None, None),
        P("row", None, None),
        P("row", "col", None),
        P("row", "col"),
        P(("row", "col"), None),
    )
    return jax.shard_map(
        local, mesh=mesh, in_specs=placed, out_specs=P(("row", "col"), None), check_vma=False
    )
```

```python
import jax
import jax.numpy as jnp
from jax import lax
from jax.experimental import pallas as pl
from jax.experimental.pallas import tpu as pltpu
from jax.sharding import PartitionSpec as P

F32, BF16, I32 = jnp.float32, jnp.bfloat16, jnp.int32
BASE = 32
TILE = 256
BIG = 512
CHUNK = 256
SLOTS = 8
GROUPS = 4
LOGICAL = pl.DeviceIdType.LOGICAL
EMPTY = -512.0


def iota(shape, axis):
    return lax.broadcasted_iota(I32, shape, axis)


def split(x):
    hi = x.astype(BF16)
    return hi, (x - hi.astype(F32)).astype(BF16)


def mm(a, b):
    return jnp.dot(a, b, preferred_element_type=F32)


def mm_nt(a, b):
    return lax.dot_general(a, b, (((1,), (1,)), ((), ())), preferred_element_type=F32)


def mm3(a, b):
    return mm(a[0], b[0]) + (mm(a[0], b[1]) + mm(a[1], b[0]))


def invert_base(strip):
    rows, width = strip.shape
    lane = iota((rows, width), 1)
    row = iota((rows, width), 0)
    within = lane % BASE
    start = lane - within
    tiles = range(0, width, 128)
    local = (lane - within)[:, :128] % 128

    def pick(x, index):
        return jnp.concatenate(
            [jnp.take_along_axis(x[:, t : t + 128], index[: x.shape[0]], axis=1) for t in tiles], axis=1
        )

    recip = 1.0 / pick(strip, local + row[:, :128])
    scaled = jnp.where(within < row, strip * recip, 0.0)
    inverse = jnp.where(within == row, recip, 0.0)
    for k in range(rows - 1):
        first = (k + 1) // 8 * 8
        factor = pick(scaled[first:], local + k)
        update = inverse[first:] - factor * inverse[k : k + 1]
        inverse = update if first == 0 else jnp.concatenate([inverse[:first], update], axis=0)
    return inverse


def spread(strip, size):
    if size == TILE:
        return strip
    group = iota((size, TILE), 1) // size
    return tuple(
        jnp.concatenate(
            [part * jnp.where(group == q, 1.0, 0.0).astype(BF16) for q in range(TILE // size)], axis=0
        )
        for part in strip
    )


def below(corner, first, second, size):
    inner = mm3(split(corner), spread(split(first), size))
    return -mm3(split(second), spread(split(inner), size))


def widen(tiles):
    return [jnp.concatenate(tiles[t : t + 2], axis=1) for t in range(0, len(tiles), 2)]


def narrow(strips):
    return [w[:, h : h + 128] for w in strips for h in (0, 128)]


def invert(diag):
    n_tile = diag.shape[0]
    small = [
        diag[t, h : h + 128, h : h + 128] for t in range(n_tile) for h in range(0, TILE, 128)
    ]
    group = iota((BASE, 128), 1) // BASE
    strips = []
    for tile in small:
        strip = tile[:BASE]
        for q in range(1, 128 // BASE):
            strip = jnp.where(group == q, tile[q * BASE : (q + 1) * BASE], strip)
        strips.append(strip)
    base = invert_base(jnp.concatenate(strips, axis=1))
    tiles = [base[:, t : t + 128] for t in range(0, base.shape[1], 128)]
    size = BASE
    while size < 128:
        group = iota((size, 128), 1) // size
        even = group % 2 == 0
        corners = []
        for tile in small:
            corner = tile[size : 2 * size]
            for q in range(1, 128 // (2 * size)):
                at = (2 * q + 1) * size
                corner = jnp.where(group == 2 * q, tile[at : at + size], corner)
            corners.append(corner)

        def evens(x):
            return [jnp.where(even, x[t], pltpu.roll(x[t + 1], size, 1)) for t in range(0, len(x), 2)]

        def odds(x):
            return [jnp.where(even, pltpu.roll(x[t], 128 - size, 1), x[t + 1]) for t in range(0, len(x), 2)]

        left = narrow(
            [
                below(c, f, g, size)
                for c, f, g in zip(widen(evens(corners)), widen(evens(tiles)), widen(odds(tiles)))
            ]
        )
        merged = []
        for t, tile in enumerate(tiles):
            x = left[t // 2] if t % 2 == 0 else pltpu.roll(left[t // 2], 128 - size, 1)
            merged.append(
                jnp.concatenate([jnp.where(even, tile, 0.0), jnp.where(even, x, tile)], axis=0)
            )
        tiles = merged
        size *= 2
    corners = [diag[t, 128:, :128] for t in range(n_tile)]
    left = narrow(
        [below(c, f, g, 128) for c, f, g in zip(widen(corners), widen(tiles[::2]), widen(tiles[1::2]))]
    )
    zero = jnp.zeros((128, 128), F32)
    return [
        jnp.concatenate(
            [
                jnp.concatenate([tiles[2 * t], zero], axis=1),
                jnp.concatenate([left[t], tiles[2 * t + 1]], axis=1),
            ],
            axis=0,
        )
        for t in range(n_tile)
    ]


def kernel(
    panel_hbm, factor_hbm, rows_hbm, target_ref, out_ref,
    panel, rows, diag, sub, off, vh, vl, oh, ol, fwd, sol, place, send, recv, send_idx, recv_idx,
    load_sem, send_sem, recv_sem,
):
    n_holders = lax.axis_size("row") * lax.axis_size("col")
    me = lax.axis_index("row") * lax.axis_size("col") + lax.axis_index("col")
    n_big = off.shape[0]
    n_tile = diag.shape[0]
    owned = out_ref.shape[0]
    pairs = [(1, 0), (2, 0), (2, 1)]
    loads = []

    def load(src, dst):
        cp = pltpu.make_async_copy(src, dst, load_sem.at[len(loads)])
        cp.start()
        loads.append(cp)
        return cp

    def factor_at(r, c, size):
        return factor_hbm.at[pl.ds(r * size, size), pl.ds(c * size, size)]

    load_diag = [load(factor_at(t, t, TILE), diag.at[t]) for t in range(n_tile)]
    load_sub = [load(factor_at(2 * t + 1, 2 * t, TILE), sub.at[t]) for t in range(n_big)]
    load_off = [load(factor_at(i, j, BIG), off.at[p]) for p, (i, j) in enumerate(pairs)]
    load_panel = load(panel_hbm, panel)
    load_rows = load(rows_hbm, rows)

    barrier = pltpu.get_barrier_semaphore()

    def device_at(o):
        return lax.rem(me + o, n_holders)

    for o in range(1, n_holders):
        pl.semaphore_signal(barrier, inc=1, device_id=device_at(o), device_id_type=LOGICAL)

    sent = target_ref.shape[1]
    target = jnp.broadcast_to(target_ref[...], (8, sent))
    holder = target // owned
    within = target - holder * owned
    lane = iota((8, sent), 1)
    rank = jnp.zeros((8, sent), I32)
    for d in range(1, SLOTS):
        same = (pltpu.roll(holder, d, 1) == holder) & (lane >= d)
        rank = rank + jnp.where(same, 1, 0)
    away = holder - me
    away = jnp.where(away < 0, away + n_holders, away)
    position = (away * SLOTS + rank)[:1]
    slots = n_holders * SLOTS
    placed = jnp.where(iota((slots, sent), 0) == position, 1.0, 0.0).astype(BF16)
    place[...] = placed
    described = jnp.concatenate(
        [jnp.broadcast_to(within[:1].astype(F32), (128, sent)), jnp.ones((128, sent), F32)], axis=0
    ).astype(BF16)
    found = mm_nt(placed, described)
    index = found[:, :128] + EMPTY * (1.0 - found[:, 128:])
    send_idx[...] = index.reshape(n_holders, SLOTS, 128)

    for cp in load_diag:
        cp.wait()
    inverse = invert(diag)
    for b in range(n_big):
        load_sub[b].wait()
        left = split(below(sub[b], inverse[2 * b], inverse[2 * b + 1], TILE))
        top, bottom = split(inverse[2 * b]), split(inverse[2 * b + 1])
        for ref, i in ((vh, 0), (vl, 1)):
            ref[b, :TILE, :TILE] = top[i]
            ref[b, TILE:, TILE:] = bottom[i]
            ref[b, TILE:, :TILE] = left[i]

    for p in range(len(pairs)):
        load_off[p].wait()
        oh[p], ol[p] = split(off[p])

    pl.semaphore_wait(barrier, n_holders - 1)

    def dispatch(source, target_buf, sem_at, offsets):
        for o in offsets:
            if o:
                pltpu.make_async_remote_copy(
                    src_ref=source.at[o],
                    dst_ref=target_buf.at[n_holders - o],
                    send_sem=send_sem.at[sem_at],
                    recv_sem=recv_sem.at[sem_at],
                    device_id=device_at(o),
                    device_id_type=LOGICAL,
                ).start()
            else:
                target_buf[0] = source[0]

    others = pl.ds(1, n_holders - 1)

    def arrived(source, target_buf, sem_at):
        pltpu.make_async_copy(source.at[others], target_buf.at[others], recv_sem.at[sem_at]).wait()

    def left_device(source, target_buf, sem_at):
        pltpu.make_async_copy(source.at[others], target_buf.at[others], send_sem.at[sem_at]).wait()

    dispatch(send_idx, recv_idx, 0, range(n_holders))

    def block_inv(b):
        return (vh[b], vl[b])

    load_panel.wait()
    n_chunk = send.shape[0]
    for ch in range(n_chunk):
        cols = slice(ch * CHUNK, (ch + 1) * CHUNK)
        rhs = [panel[b * BIG : (b + 1) * BIG, cols].astype(F32) for b in range(n_big)]
        for b in range(n_big):
            r = split(rhs[b])
            v = block_inv(b)
            upper = mm3((v[0][:TILE, :TILE], v[1][:TILE, :TILE]), (r[0][:TILE], r[1][:TILE]))
            lower = mm3((v[0][TILE:], v[1][TILE:]), r)
            f = jnp.concatenate([upper, lower], axis=0)
            fwd[:, b * BIG : (b + 1) * BIG] = f.T
            fs = split(f)
            for p, (i, j) in enumerate(pairs):
                if j == b:
                    rhs[i] = rhs[i] - mm3((oh[p], ol[p]), fs)
        for b in reversed(range(n_big)):
            q = split(fwd[:, b * BIG : (b + 1) * BIG])
            v = block_inv(b)
            first = mm3(q, (v[0][:, :TILE], v[1][:, :TILE]))
            second = mm3((q[0][:, TILE:], q[1][:, TILE:]), (v[0][TILE:, TILE:], v[1][TILE:, TILE:]))
            x = jnp.concatenate([first, second], axis=1)
            xs = split(x)
            sol[:, b * BIG : (b + 1) * BIG] = xs[0]
            for p, (i, j) in enumerate(pairs):
                if i == b:
                    at = slice(j * BIG, (j + 1) * BIG)
                    fwd[:, at] = fwd[:, at] - mm3(xs, (oh[p], ol[p]))
        if ch == 0:
            load_rows.wait()
        update = mm_nt(rows[...], sol[...]).astype(BF16)
        step = n_holders // GROUPS
        for g in range(GROUPS):
            some = slice(g * step, (g + 1) * step)
            packed = mm(place[g * step * SLOTS : (g + 1) * step * SLOTS], update).reshape(step, SLOTS, CHUNK)
            send[ch, some] = jnp.concatenate([packed[:, :, :128], packed[:, :, 128:]], axis=1).astype(BF16)
            dispatch(send.at[ch], recv.at[ch], 1 + ch, range(g * step, (g + 1) * step))

    arrived(send_idx, recv_idx, 0)
    pick0 = jnp.where(iota((8, 128), 1) == 0, 1.0, 0.0).astype(BF16)
    named = mm_nt(pick0, recv_idx[...].reshape(slots, 128).astype(BF16))[:1]
    gather = jnp.where(iota((owned, slots), 0).astype(F32) == named, 1.0, 0.0).astype(BF16)
    for ch in range(n_chunk):
        arrived(send.at[ch], recv.at[ch], 1 + ch)
        got = recv[ch].astype(F32)
        got = jnp.concatenate([got[:, :SLOTS].reshape(slots, 128), got[:, SLOTS:].reshape(slots, 128)], axis=1)
        out_ref[:, ch * CHUNK : (ch + 1) * CHUNK] = mm(gather, got.astype(BF16))
    left_device(send_idx, recv_idx, 0)
    for ch in range(n_chunk):
        left_device(send.at[ch], recv.at[ch], 1 + ch)


def local(coupling_panel, interior_factor, border_rows, target_rows, border_block):
    panel, factor, rows = coupling_panel[0], interior_factor[0], border_rows[0]
    n, width = panel.shape
    holders = lax.axis_size("row") * lax.axis_size("col")
    n_tile, n_big, n_chunk = n // TILE, n // BIG, width // CHUNK
    pairs = n_big * (n_big - 1) // 2
    vmem = pl.BlockSpec(memory_space=pltpu.VMEM)
    hbm = pl.BlockSpec(memory_space=pl.ANY)
    assembled = pl.pallas_call(
        kernel,
        out_shape=jax.ShapeDtypeStruct(border_block.shape, F32),
        in_specs=[hbm, hbm, hbm, vmem],
        out_specs=vmem,
        scratch_shapes=[
            pltpu.VMEM(panel.shape, BF16),
            pltpu.VMEM(rows.shape, BF16),
            pltpu.VMEM((n_tile, TILE, TILE), F32),
            pltpu.VMEM((n_big, TILE, TILE), F32),
            pltpu.VMEM((pairs, BIG, BIG), F32),
            pltpu.VMEM((n_big, BIG, BIG), BF16),
            pltpu.VMEM((n_big, BIG, BIG), BF16),
            pltpu.VMEM((pairs, BIG, BIG), BF16),
            pltpu.VMEM((pairs, BIG, BIG), BF16),
            pltpu.VMEM((CHUNK, n), F32),
            pltpu.VMEM((CHUNK, n), BF16),
            pltpu.VMEM((holders * SLOTS, target_rows.shape[1]), BF16),
            pltpu.VMEM((n_chunk, holders, 2 * SLOTS, 128), BF16),
            pltpu.VMEM((n_chunk, holders, 2 * SLOTS, 128), BF16),
            pltpu.VMEM((holders, SLOTS, 128), F32),
            pltpu.VMEM((holders, SLOTS, 128), F32),
            pltpu.SemaphoreType.DMA((n_tile + n_big + pairs + 2,)),
            pltpu.SemaphoreType.DMA((1 + n_chunk,)),
            pltpu.SemaphoreType.DMA((1 + n_chunk,)),
        ],
        compiler_params=pltpu.CompilerParams(
            collective_id=0, has_side_effects=True, vmem_limit_bytes=60 * 1024 * 1024
        ),
        name="schur_panel",
    )(panel, factor, rows, target_rows)
    return border_block - assembled


def solution(mesh):
    placed = (
        P("row", None, None),
        P("row", None, None),
        P("row", "col", None),
        P("row", "col"),
        P(("row", "col"), None),
    )
    return jax.shard_map(
        local, mesh=mesh, in_specs=placed, out_specs=P(("row", "col"), None), check_vma=False
    )
```

```python
import jax
import jax.numpy as jnp
from jax import lax
from jax.experimental import pallas as pl
from jax.experimental.pallas import tpu as pltpu
from jax.sharding import PartitionSpec as P

F32, BF16, I32 = jnp.float32, jnp.bfloat16, jnp.int32
BASE = 32
TILE = 256
BIG = 512
CHUNK = 256
SLOTS = 8
GROUPS = 2
LOGICAL = pl.DeviceIdType.LOGICAL
EMPTY = -512.0


def iota(shape, axis):
    return lax.broadcasted_iota(I32, shape, axis)


def split(x):
    hi = x.astype(BF16)
    return hi, (x - hi.astype(F32)).astype(BF16)


def mm(a, b):
    return jnp.dot(a, b, preferred_element_type=F32)


def mm_nt(a, b):
    return lax.dot_general(a, b, (((1,), (1,)), ((), ())), preferred_element_type=F32)


def mm3(a, b):
    return mm(a[0], b[0]) + (mm(a[0], b[1]) + mm(a[1], b[0]))


def invert_base(strip):
    rows, width = strip.shape
    lane = iota((rows, width), 1)
    row = iota((rows, width), 0)
    within = lane % BASE
    start = lane - within
    tiles = range(0, width, 128)
    local = (lane - within)[:, :128] % 128

    def pick(x, index):
        return jnp.concatenate(
            [jnp.take_along_axis(x[:, t : t + 128], index[: x.shape[0]], axis=1) for t in tiles], axis=1
        )

    recip = 1.0 / pick(strip, local + row[:, :128])
    scaled = jnp.where(within < row, strip * recip, 0.0)
    inverse = jnp.where(within == row, recip, 0.0)
    for k in range(rows - 1):
        first = (k + 1) // 8 * 8
        factor = pick(scaled[first:], local + k)
        update = inverse[first:] - factor * inverse[k : k + 1]
        inverse = update if first == 0 else jnp.concatenate([inverse[:first], update], axis=0)
    return inverse


def spread(strip, size):
    if size == TILE:
        return strip
    group = iota((size, TILE), 1) // size
    return tuple(
        jnp.concatenate(
            [part * jnp.where(group == q, 1.0, 0.0).astype(BF16) for q in range(TILE // size)], axis=0
        )
        for part in strip
    )


def below(corner, first, second, size):
    inner = mm3(split(corner), spread(split(first), size))
    return mm3(split(second), spread(split(inner), size))


def widen(tiles):
    return [jnp.concatenate(tiles[t : t + 2], axis=1) for t in range(0, len(tiles), 2)]


def narrow(strips):
    return [w[:, h : h + 128] for w in strips for h in (0, 128)]


def invert(diag):
    n_tile = diag.shape[0]
    small = [
        diag[t, h : h + 128, h : h + 128] for t in range(n_tile) for h in range(0, TILE, 128)
    ]
    group = iota((BASE, 128), 1) // BASE
    strips = []
    for tile in small:
        strip = tile[:BASE]
        for q in range(1, 128 // BASE):
            strip = jnp.where(group == q, tile[q * BASE : (q + 1) * BASE], strip)
        strips.append(strip)
    base = invert_base(jnp.concatenate(strips, axis=1))
    tiles = [base[:, t : t + 128] for t in range(0, base.shape[1], 128)]
    size = BASE
    while size < 128:
        group = iota((size, 128), 1) // size
        even = group % 2 == 0
        corners = []
        for tile in small:
            corner = tile[size : 2 * size]
            for q in range(1, 128 // (2 * size)):
                at = (2 * q + 1) * size
                corner = jnp.where(group == 2 * q, tile[at : at + size], corner)
            corners.append(corner)

        def evens(x):
            return [jnp.where(even, x[t], pltpu.roll(x[t + 1], size, 1)) for t in range(0, len(x), 2)]

        def odds(x):
            return [jnp.where(even, pltpu.roll(x[t], 128 - size, 1), x[t + 1]) for t in range(0, len(x), 2)]

        left = narrow(
            [
                below(c, f, g, size)
                for c, f, g in zip(widen(evens(corners)), widen(evens(tiles)), widen(odds(tiles)))
            ]
        )
        merged = []
        for t, tile in enumerate(tiles):
            x = left[t // 2] if t % 2 == 0 else pltpu.roll(left[t // 2], 128 - size, 1)
            merged.append(
                jnp.concatenate([jnp.where(even, tile, 0.0), jnp.where(even, -x, tile)], axis=0)
            )
        tiles = merged
        size *= 2
    corners = [diag[t, 128:, :128] for t in range(n_tile)]
    left = narrow(
        [below(c, f, g, 128) for c, f, g in zip(widen(corners), widen(tiles[::2]), widen(tiles[1::2]))]
    )
    zero = jnp.zeros((128, 128), F32)
    return [
        jnp.concatenate(
            [
                jnp.concatenate([tiles[2 * t], zero], axis=1),
                jnp.concatenate([-left[t], tiles[2 * t + 1]], axis=1),
            ],
            axis=0,
        )
        for t in range(n_tile)
    ]


def kernel(
    panel_hbm, factor_hbm, rows_hbm, target_ref, out_ref,
    panel, rows, diag, sub, off, vh, vl, oh, ol, fwd, place, send0, recv0, send1, recv1,
    load_sem, send_sem, recv_sem,
):
    n_holders = lax.axis_size("row") * lax.axis_size("col")
    me = lax.axis_index("row") * lax.axis_size("col") + lax.axis_index("col")
    n_big = off.shape[0]
    n_tile = diag.shape[0]
    owned = out_ref.shape[0]
    sends, recvs = (send0, send1), (recv0, recv1)
    pairs = [(1, 0), (2, 0), (2, 1)]
    loads = []

    def load(src, dst):
        cp = pltpu.make_async_copy(src, dst, load_sem.at[len(loads)])
        cp.start()
        loads.append(cp)

    def factor_at(r, c, size):
        return factor_hbm.at[pl.ds(r * size, size), pl.ds(c * size, size)]

    for t in range(n_tile):
        load(factor_at(t, t, TILE), diag.at[t])
    for t in range(n_big):
        load(factor_at(2 * t + 1, 2 * t, TILE), sub.at[t])
    for p, (i, j) in enumerate(pairs):
        load(factor_at(i, j, BIG), off.at[p])
    load(panel_hbm, panel)
    load(rows_hbm, rows)

    with jax.named_scope("greet"):
        barrier = pltpu.get_barrier_semaphore()

        def device_at(o):
            return lax.rem(me + o, n_holders)

        for o in range(1, n_holders):
            pl.semaphore_signal(barrier, inc=1, device_id=device_at(o), device_id_type=LOGICAL)

    for cp in loads[:-2]:
        cp.wait()

    with jax.named_scope("invert"):
        sent = target_ref.shape[1]
        target = jnp.broadcast_to(target_ref[...], (8, sent))
        holder = target // owned
        within = target - holder * owned
        lane = iota((8, sent), 1)
        rank = jnp.zeros((8, sent), I32)
        for d in range(1, SLOTS):
            same = (pltpu.roll(holder, d, 1) == holder) & (lane >= d)
            rank = rank + jnp.where(same, 1, 0)
        away = holder - me
        away = jnp.where(away < 0, away + n_holders, away)
        position = (away * SLOTS + rank)[:1]
        slots = n_holders * SLOTS
        placed = jnp.where(iota((slots, sent), 0) == position, 1.0, 0.0).astype(BF16)
        place[...] = placed
        described = jnp.concatenate(
            [jnp.broadcast_to(within[:1].astype(F32), (128, sent)), jnp.ones((128, sent), F32)], axis=0
        ).astype(BF16)
        found = mm_nt(placed, described)
        index = found[:, :128] + EMPTY * (1.0 - found[:, 128:])
        send0[:, 2 * SLOTS :] = index.reshape(n_holders, SLOTS, 128).astype(BF16)

        inverse = invert(diag)
        for b in range(n_big):
            left = split(below(sub[b], inverse[2 * b], inverse[2 * b + 1], TILE))
            top, bottom = split(inverse[2 * b]), split(inverse[2 * b + 1])
            for ref, i in ((vh, 0), (vl, 1)):
                ref[b, 0] = top[i]
                ref[b, 1] = left[i]
                ref[b, 2] = bottom[i]
        for p in range(len(pairs)):
            oh[p], ol[p] = split(off[p])

    loads[-2].wait()
    loads[-1].wait()
    with jax.named_scope("barwait"):
        pl.semaphore_wait(barrier, n_holders - 1)

    def dispatch(ch):
        for o in range(1, n_holders):
            pltpu.make_async_remote_copy(
                src_ref=sends[ch].at[o],
                dst_ref=recvs[ch].at[n_holders - o],
                send_sem=send_sem.at[ch],
                recv_sem=recv_sem.at[ch],
                device_id=device_at(o),
                device_id_type=LOGICAL,
            ).start()
        recvs[ch][0] = sends[ch][0]

    others = pl.ds(1, n_holders - 1)

    def arrived(ch):
        pltpu.make_async_copy(sends[ch].at[others], recvs[ch].at[others], recv_sem.at[ch]).wait()

    def left_device(ch):
        pltpu.make_async_copy(sends[ch].at[others], recvs[ch].at[others], send_sem.at[ch]).wait()

    def inv(b, part):
        return (vh[b, part], vl[b, part])

    def halves(x, axis):
        if axis == 0:
            return [tuple(y[:TILE] for y in x), tuple(y[TILE:] for y in x)]
        return [tuple(y[:, :TILE] for y in x), tuple(y[:, TILE:] for y in x)]

    n_chunk = len(sends)
    for ch in range(n_chunk):
        with jax.named_scope("fwd"):
            cols = slice(ch * CHUNK, (ch + 1) * CHUNK)
            rhs = [panel[b * BIG : (b + 1) * BIG, cols].astype(F32) for b in range(n_big)]
            for b in range(n_big):
                r = halves(split(rhs[b]), 0)
                upper = mm3(inv(b, 0), r[0])
                lower = mm3(inv(b, 2), r[1]) - mm3(inv(b, 1), r[0])
                f = jnp.concatenate([upper, lower], axis=0)
                fwd[:, b * BIG : (b + 1) * BIG] = f.T
                fs = halves(split(f), 0)
                for p, (i, j) in enumerate(pairs):
                    if j == b:
                        o = halves((oh[p], ol[p]), 1)
                        rhs[i] = (rhs[i] - mm3(o[0], fs[0])) - mm3(o[1], fs[1])
        with jax.named_scope("bwd"):
            partial = []
            for b in reversed(range(n_big)):
                q = halves(split(fwd[:, b * BIG : (b + 1) * BIG]), 1)
                first = mm3(q[0], inv(b, 0)) - mm3(q[1], inv(b, 1))
                second = mm3(q[1], inv(b, 2))
                x = jnp.concatenate([first, second], axis=1)
                xs = halves(split(x), 1)
                for p, (i, j) in reversed(list(enumerate(pairs))):
                    if i == b:
                        at = slice(j * BIG, (j + 1) * BIG)
                        o = halves((oh[p], ol[p]), 0)
                        fwd[:, at] = (fwd[:, at] - mm3(xs[0], o[0])) - mm3(xs[1], o[1])
                at = b * BIG
                if b:
                    partial.append(mm_nt(rows[:, at : at + BIG], jnp.concatenate([-xs[0][0], -xs[1][0]], axis=1)))
                else:
                    update = mm_nt(rows[:, :TILE], xs[0][0]) - mm_nt(rows[:, TILE:BIG], -xs[1][0])
            for other in partial:
                update = update - other
            update = update.astype(BF16)
        with jax.named_scope("pack"):
            step = n_holders // GROUPS
            for g in range(GROUPS):
                some = slice(g * step, (g + 1) * step)
                packed = mm(place[g * step * SLOTS : (g + 1) * step * SLOTS], update).reshape(step, SLOTS, CHUNK)
                packed = jnp.concatenate([packed[:, :, :128], packed[:, :, 128:]], axis=1).astype(BF16)
                sends[ch][some, : 2 * SLOTS] = packed
        with jax.named_scope("send"):
            dispatch(ch)

    for ch in range(n_chunk):
        with jax.named_scope("wait"):
            arrived(ch)
        with jax.named_scope("final"):
            if ch == 0:
                pick0 = jnp.where(iota((8, 128), 1) == 0, 1.0, 0.0).astype(BF16)
                named = mm_nt(pick0, recv0[:, 2 * SLOTS :].astype(F32).reshape(slots, 128).astype(BF16))[:1]
                gather = jnp.where(iota((owned, slots), 0).astype(F32) == named, 1.0, 0.0).astype(BF16)
            got = recvs[ch][:, : 2 * SLOTS].astype(F32)
            got = jnp.concatenate(
                [got[:, :SLOTS].reshape(slots, 128), got[:, SLOTS:].reshape(slots, 128)], axis=1
            )
            out_ref[:, ch * CHUNK : (ch + 1) * CHUNK] = mm(gather, got.astype(BF16))
    for ch in range(n_chunk):
        left_device(ch)


def local(coupling_panel, interior_factor, border_rows, target_rows, border_block):
    panel, factor, rows = coupling_panel[0], interior_factor[0], border_rows[0]
    n, width = panel.shape
    holders = lax.axis_size("row") * lax.axis_size("col")
    n_tile, n_big, n_chunk = n // TILE, n // BIG, width // CHUNK
    pairs = n_big * (n_big - 1) // 2
    vmem = pl.BlockSpec(memory_space=pltpu.VMEM)
    hbm = pl.BlockSpec(memory_space=pl.ANY)
    assembled = pl.pallas_call(
        kernel,
        out_shape=jax.ShapeDtypeStruct(border_block.shape, F32),
        in_specs=[hbm, hbm, hbm, vmem],
        out_specs=vmem,
        scratch_shapes=[
            pltpu.VMEM(panel.shape, BF16),
            pltpu.VMEM(rows.shape, BF16),
            pltpu.VMEM((n_tile, TILE, TILE), F32),
            pltpu.VMEM((n_big, TILE, TILE), F32),
            pltpu.VMEM((pairs, BIG, BIG), F32),
            pltpu.VMEM((n_big, 3, TILE, TILE), BF16),
            pltpu.VMEM((n_big, 3, TILE, TILE), BF16),
            pltpu.VMEM((pairs, BIG, BIG), BF16),
            pltpu.VMEM((pairs, BIG, BIG), BF16),
            pltpu.VMEM((CHUNK, n), F32),
            pltpu.VMEM((holders * SLOTS, target_rows.shape[1]), BF16),
            pltpu.VMEM((holders, 3 * SLOTS, 128), BF16),
            pltpu.VMEM((holders, 3 * SLOTS, 128), BF16),
            pltpu.VMEM((holders, 2 * SLOTS, 128), BF16),
            pltpu.VMEM((holders, 2 * SLOTS, 128), BF16),
            pltpu.SemaphoreType.DMA((n_tile + n_big + pairs + 2,)),
            pltpu.SemaphoreType.DMA((n_chunk,)),
            pltpu.SemaphoreType.DMA((n_chunk,)),
        ],
        compiler_params=pltpu.CompilerParams(
            collective_id=0, has_side_effects=True, vmem_limit_bytes=60 * 1024 * 1024
        ),
        name="schur_panel",
    )(panel, factor, rows, target_rows)
    return border_block - assembled


def solution(mesh):
    placed = (
        P("row", None, None),
        P("row", None, None),
        P("row", "col", None),
        P("row", "col"),
        P(("row", "col"), None),
    )
    return jax.shard_map(
        local, mesh=mesh, in_specs=placed, out_specs=P(("row", "col"), None), check_vma=False
    )
```

```python
import jax
import jax.numpy as jnp
from jax import lax
from jax.experimental import pallas as pl
from jax.experimental.pallas import tpu as pltpu
from jax.sharding import PartitionSpec as P

F32, BF16, I32 = jnp.float32, jnp.bfloat16, jnp.int32
BASE = 16
TILE = 256
BIG = 512
CHUNK = 256
SLOTS = 8
GROUPS = 2
SIDE = 4
CORES = 2
LOGICAL = pl.DeviceIdType.LOGICAL
EMPTY = -512.0


def iota(shape, axis):
    return lax.broadcasted_iota(I32, shape, axis)


def split(x):
    hi = x.astype(BF16)
    return hi, (x - hi.astype(F32)).astype(BF16)


def mm(a, b):
    return jnp.dot(a, b, preferred_element_type=F32)


def mm_nt(a, b):
    return lax.dot_general(a, b, (((1,), (1,)), ((), ())), preferred_element_type=F32)


def mm3(a, b):
    return mm(a[0], b[0]) + (mm(a[0], b[1]) + mm(a[1], b[0]))


def invert_base(strip):
    rows, width = strip.shape
    lane = iota((rows, width), 1)
    row = iota((rows, width), 0)
    within = lane % BASE
    start = lane - within
    tiles = range(0, width, 128)
    local = (lane - within)[:, :128] % 128

    def pick(x, index):
        return jnp.concatenate(
            [jnp.take_along_axis(x[:, t : t + 128], index[: x.shape[0]], axis=1) for t in tiles], axis=1
        )

    recip = 1.0 / pick(strip, local + row[:, :128])
    scaled = jnp.where(within < row, strip * recip, 0.0)
    inverse = jnp.where(within == row, recip, 0.0)
    for k in range(rows - 1):
        first = (k + 1) // 8 * 8
        factor = pick(scaled[first:], local + k)
        update = inverse[first:] - factor * inverse[k : k + 1]
        inverse = update if first == 0 else jnp.concatenate([inverse[:first], update], axis=0)
    return inverse


def spread(strip, size):
    if size == TILE:
        return strip
    group = iota((size, TILE), 1) // size
    return tuple(
        jnp.concatenate(
            [part * jnp.where(group == q, 1.0, 0.0).astype(BF16) for q in range(TILE // size)], axis=0
        )
        for part in strip
    )


def below(corner, first, second, size):
    inner = mm3(split(corner), spread(split(first), size))
    return mm3(split(second), spread(split(inner), size))


def widen(tiles):
    return [jnp.concatenate(tiles[t : t + 2], axis=1) for t in range(0, len(tiles), 2)]


def narrow(strips):
    return [w[:, h : h + 128] for w in strips for h in (0, 128)]


def small_tiles(diag):
    return [diag[t, h : h + 128, h : h + 128] for t in range(diag.shape[0]) for h in range(0, TILE, 128)]


def invert_bases(diag):
    small = small_tiles(diag)
    group = iota((BASE, 128), 1) // BASE
    strips = []
    for tile in small:
        strip = tile[:BASE]
        for q in range(1, 128 // BASE):
            strip = jnp.where(group == q, tile[q * BASE : (q + 1) * BASE], strip)
        strips.append(strip)
    base = invert_base(jnp.concatenate(strips, axis=1))
    return [base[:, t : t + 128] for t in range(0, base.shape[1], 128)]


def invert(diag, tiles):
    n_tile = diag.shape[0]
    small = small_tiles(diag)
    size = BASE
    while size < 128:
        group = iota((size, 128), 1) // size
        even = group % 2 == 0
        corners = []
        for tile in small:
            corner = tile[size : 2 * size]
            for q in range(1, 128 // (2 * size)):
                at = (2 * q + 1) * size
                corner = jnp.where(group == 2 * q, tile[at : at + size], corner)
            corners.append(corner)

        def evens(x):
            return [jnp.where(even, x[t], pltpu.roll(x[t + 1], size, 1)) for t in range(0, len(x), 2)]

        def odds(x):
            return [jnp.where(even, pltpu.roll(x[t], 128 - size, 1), x[t + 1]) for t in range(0, len(x), 2)]

        left = narrow(
            [
                below(c, f, g, size)
                for c, f, g in zip(widen(evens(corners)), widen(evens(tiles)), widen(odds(tiles)))
            ]
        )
        merged = []
        for t, tile in enumerate(tiles):
            x = left[t // 2] if t % 2 == 0 else pltpu.roll(left[t // 2], 128 - size, 1)
            merged.append(
                jnp.concatenate([jnp.where(even, tile, 0.0), jnp.where(even, -x, tile)], axis=0)
            )
        tiles = merged
        size *= 2
    corners = [diag[t, 128:, :128] for t in range(n_tile)]
    left = narrow(
        [below(c, f, g, 128) for c, f, g in zip(widen(corners), widen(tiles[::2]), widen(tiles[1::2]))]
    )
    zero = jnp.zeros((128, 128), F32)
    return [
        jnp.concatenate(
            [
                jnp.concatenate([tiles[2 * t], zero], axis=1),
                jnp.concatenate([-left[t], tiles[2 * t + 1]], axis=1),
            ],
            axis=0,
        )
        for t in range(n_tile)
    ]


def parts_of(device):
    col = SIDE * SIDE
    return (
        lax.div(device, CORES * col),
        lax.rem(lax.div(device, col), CORES),
        lax.rem(lax.div(device, SIDE), SIDE),
        lax.rem(device, SIDE),
    )


def joined(y, core, x, z):
    return ((y * CORES + core) * SIDE + x) * SIDE + z


SIZES = (SIDE, CORES, SIDE, SIDE)


def steps_of(offset):
    return (
        offset // (CORES * SIDE * SIDE),
        offset // (SIDE * SIDE) % CORES,
        offset // SIDE % SIDE,
        offset % SIDE,
    )


def opposite(offset):
    return joined(*((n - d) % n for n, d in zip(SIZES, steps_of(offset))))


def hops(offset):
    y, core, x, z = steps_of(offset)
    return sum(min(d, SIDE - d) for d in (y, x, z)) + 0.5 * core


def kernel(
    panel_hbm, factor_hbm, rows_hbm, target_hbm, out_ref,
    panel, rows, diag, sub, off, vh, vl, oh, ol, fwd, place, send0, recv0, send1, recv1, target_ref, result,
    load_sem, send_sem, recv_sem,
):
    n_holders = lax.axis_size("row") * lax.axis_size("col")
    me = lax.axis_index("row") * lax.axis_size("col") + lax.axis_index("col")
    here = parts_of(me)
    n_big = off.shape[0]
    n_tile = diag.shape[0]
    owned = result.shape[0]
    sends, recvs = (send0, send1), (recv0, recv1)
    pairs = [(1, 0), (2, 0), (2, 1)]
    offsets = sorted(range(1, n_holders), key=lambda o: -hops(o))
    ahead = [[lax.rem(c + d, n) for d in range(n)] for c, n in zip(here, SIZES)]
    rows_ahead = [joined(y, core, 0, 0) for y in ahead[0] for core in ahead[1]]
    cols_ahead = [joined(0, 0, x, z) for x in ahead[2] for z in ahead[3]]

    def device_at(o):
        return rows_ahead[o // (SIDE * SIDE)] + cols_ahead[o % (SIDE * SIDE)]

    loads = []

    def load(src, dst):
        cp = pltpu.make_async_copy(src, dst, load_sem.at[len(loads)])
        cp.start()
        loads.append(cp)

    def factor_at(r, c, size):
        return factor_hbm.at[pl.ds(r * size, size), pl.ds(c * size, size)]

    for t in range(n_tile):
        load(factor_at(t, t, TILE), diag.at[t])
    for t in range(n_big):
        load(factor_at(2 * t + 1, 2 * t, TILE), sub.at[t])
    for p, (i, j) in enumerate(pairs):
        load(factor_at(i, j, BIG), off.at[p])
    load(target_hbm, target_ref)
    load(panel_hbm, panel)
    load(rows_hbm, rows)

    with jax.named_scope("greet"):
        barrier = pltpu.get_barrier_semaphore()
        for o in offsets:
            pl.semaphore_signal(barrier, inc=1, device_id=device_at(o), device_id_type=LOGICAL)

    for cp in loads[:n_tile]:
        cp.wait()
    with jax.named_scope("base"):
        base = invert_bases(diag)
    for cp in loads[n_tile:-2]:
        cp.wait()

    with jax.named_scope("invert"):
        sent = target_ref.shape[1]
        target = jnp.broadcast_to(target_ref[...], (8, sent))
        holder = target // owned
        within = target - holder * owned
        lane = iota((8, sent), 1)
        rank = jnp.zeros((8, sent), I32)
        for d in range(1, SLOTS):
            same = (pltpu.roll(holder, d, 1) == holder) & (lane >= d)
            rank = rank + jnp.where(same, 1, 0)
        away = joined(*(lax.rem(h - c + n, n) for h, c, n in zip(parts_of(holder), here, SIZES)))
        position = (away * SLOTS + rank)[:1]
        slots = n_holders * SLOTS
        placed = jnp.where(iota((slots, sent), 0) == position, 1.0, 0.0).astype(BF16)
        place[...] = placed
        described = jnp.concatenate(
            [jnp.broadcast_to(within[:1].astype(F32), (128, sent)), jnp.ones((128, sent), F32)], axis=0
        ).astype(BF16)
        found = mm_nt(placed, described)
        index = found[:, :128] + EMPTY * (1.0 - found[:, 128:])
        send0[:, 2 * SLOTS :] = index.reshape(n_holders, SLOTS, 128).astype(BF16)

        inverse = invert(diag, base)
        for b in range(n_big):
            left = split(below(sub[b], inverse[2 * b], inverse[2 * b + 1], TILE))
            top, bottom = split(inverse[2 * b]), split(inverse[2 * b + 1])
            for ref, i in ((vh, 0), (vl, 1)):
                ref[b, 0] = top[i]
                ref[b, 1] = left[i]
                ref[b, 2] = bottom[i]
        for p in range(len(pairs)):
            oh[p], ol[p] = split(off[p])

    loads[-2].wait()
    loads[-1].wait()
    with jax.named_scope("barwait"):
        pl.semaphore_wait(barrier, n_holders - 1)

    def dispatch(ch):
        for o in offsets:
            pltpu.make_async_remote_copy(
                src_ref=sends[ch].at[o],
                dst_ref=recvs[ch].at[opposite(o)],
                send_sem=send_sem.at[ch],
                recv_sem=recv_sem.at[ch],
                device_id=device_at(o),
                device_id_type=LOGICAL,
            ).start()
        recvs[ch][0] = sends[ch][0]

    others = pl.ds(1, n_holders - 1)

    def arrived(ch):
        pltpu.make_async_copy(sends[ch].at[others], recvs[ch].at[others], recv_sem.at[ch]).wait()

    def left_device(ch):
        pltpu.make_async_copy(sends[ch].at[others], recvs[ch].at[others], send_sem.at[ch]).wait()

    def inv(b, part):
        return (vh[b, part], vl[b, part])

    def halves(x, axis):
        if axis == 0:
            return [tuple(y[:TILE] for y in x), tuple(y[TILE:] for y in x)]
        return [tuple(y[:, :TILE] for y in x), tuple(y[:, TILE:] for y in x)]

    n_chunk = len(sends)
    for ch in range(n_chunk):
        with jax.named_scope("fwd"):
            cols = slice(ch * CHUNK, (ch + 1) * CHUNK)
            rhs = [panel[b * BIG : (b + 1) * BIG, cols].astype(F32) for b in range(n_big)]
            for b in range(n_big):
                r = halves(split(rhs[b]), 0)
                upper = mm3(inv(b, 0), r[0])
                lower = mm3(inv(b, 2), r[1]) - mm3(inv(b, 1), r[0])
                f = jnp.concatenate([upper, lower], axis=0)
                fwd[:, b * BIG : (b + 1) * BIG] = f.T
                fs = halves(split(f), 0)
                for p, (i, j) in enumerate(pairs):
                    if j == b:
                        o = halves((oh[p], ol[p]), 1)
                        rhs[i] = (rhs[i] - mm3(o[0], fs[0])) - mm3(o[1], fs[1])
        with jax.named_scope("bwd"):
            partial = []
            for b in reversed(range(n_big)):
                q = halves(split(fwd[:, b * BIG : (b + 1) * BIG]), 1)
                first = mm3(q[0], inv(b, 0)) - mm3(q[1], inv(b, 1))
                second = mm3(q[1], inv(b, 2))
                x = jnp.concatenate([first, second], axis=1)
                xs = halves(split(x), 1)
                for p, (i, j) in reversed(list(enumerate(pairs))):
                    if i == b:
                        at = slice(j * BIG, (j + 1) * BIG)
                        o = halves((oh[p], ol[p]), 0)
                        fwd[:, at] = (fwd[:, at] - mm3(xs[0], o[0])) - mm3(xs[1], o[1])
                at = b * BIG
                if b:
                    partial.append(mm_nt(rows[:, at : at + BIG], jnp.concatenate([-xs[0][0], -xs[1][0]], axis=1)))
                else:
                    update = mm_nt(rows[:, :TILE], xs[0][0]) - mm_nt(rows[:, TILE:BIG], -xs[1][0])
            for other in partial:
                update = update - other
            update = update.astype(BF16)
        with jax.named_scope("pack"):
            step = n_holders // GROUPS
            for g in range(GROUPS):
                some = slice(g * step, (g + 1) * step)
                packed = mm(place[g * step * SLOTS : (g + 1) * step * SLOTS], update).reshape(step, SLOTS, CHUNK)
                packed = jnp.concatenate([packed[:, :, :128], packed[:, :, 128:]], axis=1).astype(BF16)
                sends[ch][some, : 2 * SLOTS] = packed
        with jax.named_scope("send"):
            dispatch(ch)

    stores = []
    for ch in range(n_chunk):
        with jax.named_scope("wait"):
            arrived(ch)
        with jax.named_scope("final"):
            if ch == 0:
                pick0 = jnp.where(iota((8, 128), 1) == 0, 1.0, 0.0).astype(BF16)
                named = mm_nt(pick0, recv0[:, 2 * SLOTS :].astype(F32).reshape(slots, 128).astype(BF16))[:1]
                gather = jnp.where(iota((owned, slots), 0).astype(F32) == named, 1.0, 0.0).astype(BF16)
            got = recvs[ch][:, : 2 * SLOTS].astype(F32)
            got = jnp.concatenate(
                [got[:, :SLOTS].reshape(slots, 128), got[:, SLOTS:].reshape(slots, 128)], axis=1
            )
            cols = pl.ds(ch * CHUNK, CHUNK)
            result[:, cols] = mm(gather, got.astype(BF16))
        store = pltpu.make_async_copy(result.at[:, cols], out_ref.at[:, cols], load_sem.at[ch])
        store.start()
        stores.append(store)
    for ch in range(n_chunk):
        left_device(ch)
        stores[ch].wait()


def local(coupling_panel, interior_factor, border_rows, target_rows, border_block):
    panel, factor, rows = coupling_panel[0], interior_factor[0], border_rows[0]
    n, width = panel.shape
    holders = lax.axis_size("row") * lax.axis_size("col")
    n_tile, n_big, n_chunk = n // TILE, n // BIG, width // CHUNK
    pairs = n_big * (n_big - 1) // 2
    hbm = pl.BlockSpec(memory_space=pl.ANY)
    assembled = pl.pallas_call(
        kernel,
        out_shape=jax.ShapeDtypeStruct(border_block.shape, F32),
        in_specs=[hbm] * 4,
        out_specs=hbm,
        scratch_shapes=[
            pltpu.VMEM(panel.shape, BF16),
            pltpu.VMEM(rows.shape, BF16),
            pltpu.VMEM((n_tile, TILE, TILE), F32),
            pltpu.VMEM((n_big, TILE, TILE), F32),
            pltpu.VMEM((pairs, BIG, BIG), F32),
            pltpu.VMEM((n_big, 3, TILE, TILE), BF16),
            pltpu.VMEM((n_big, 3, TILE, TILE), BF16),
            pltpu.VMEM((pairs, BIG, BIG), BF16),
            pltpu.VMEM((pairs, BIG, BIG), BF16),
            pltpu.VMEM((CHUNK, n), F32),
            pltpu.VMEM((holders * SLOTS, target_rows.shape[1]), BF16),
            pltpu.VMEM((holders, 3 * SLOTS, 128), BF16),
            pltpu.VMEM((holders, 3 * SLOTS, 128), BF16),
            pltpu.VMEM((holders, 2 * SLOTS, 128), BF16),
            pltpu.VMEM((holders, 2 * SLOTS, 128), BF16),
            pltpu.VMEM(target_rows.shape, I32),
            pltpu.VMEM(border_block.shape, F32),
            pltpu.SemaphoreType.DMA((n_tile + n_big + pairs + 3,)),
            pltpu.SemaphoreType.DMA((n_chunk,)),
            pltpu.SemaphoreType.DMA((n_chunk,)),
        ],
        compiler_params=pltpu.CompilerParams(
            collective_id=0, has_side_effects=True, vmem_limit_bytes=53 * 1024 * 1024
        ),
        name="schur_panel",
    )(panel, factor, rows, target_rows)
    return border_block - assembled


def solution(mesh):
    placed = (
        P("row", None, None),
        P("row", None, None),
        P("row", "col", None),
        P("row", "col"),
        P(("row", "col"), None),
    )
    return jax.shard_map(
        local, mesh=mesh, in_specs=placed, out_specs=P(("row", "col"), None), check_vma=False
    )
```

```python
import jax
import jax.numpy as jnp
from jax import lax
from jax.experimental import pallas as pl
from jax.experimental.pallas import tpu as pltpu
from jax.sharding import PartitionSpec as P

F32, BF16, I32 = jnp.float32, jnp.bfloat16, jnp.int32
BASE = 16
TILE = 256
BIG = 512
CHUNK = 256
SLOTS = 8
GROUPS = 2
SIDE = 4
CORES = 2
LOGICAL = pl.DeviceIdType.LOGICAL
EMPTY = -512.0


def iota(shape, axis):
    return lax.broadcasted_iota(I32, shape, axis)


def split(x):
    hi = x.astype(BF16)
    return hi, (x - hi.astype(F32)).astype(BF16)


def mm(a, b):
    return jnp.dot(a, b, preferred_element_type=F32)


def mm_nt(a, b):
    return lax.dot_general(a, b, (((1,), (1,)), ((), ())), preferred_element_type=F32)


def mm3(a, b):
    return mm(a[0], b[0]) + (mm(a[0], b[1]) + mm(a[1], b[0]))


def invert_base(strip):
    rows, width = strip.shape
    lane = iota((rows, width), 1)
    row = iota((rows, width), 0)
    within = lane % BASE
    start = lane - within
    tiles = range(0, width, 128)
    local = (lane - within)[:, :128] % 128

    def pick(x, index):
        return jnp.concatenate(
            [jnp.take_along_axis(x[:, t : t + 128], index[: x.shape[0]], axis=1) for t in tiles], axis=1
        )

    recip = 1.0 / pick(strip, local + row[:, :128])
    scaled = jnp.where(within < row, strip * recip, 0.0)
    inverse = jnp.where(within == row, recip, 0.0)
    for k in range(rows - 1):
        first = (k + 1) // 8 * 8
        factor = pick(scaled[first:], local + k)
        update = inverse[first:] - factor * inverse[k : k + 1]
        inverse = update if first == 0 else jnp.concatenate([inverse[:first], update], axis=0)
    return inverse


def spread(strip, size):
    if size == TILE:
        return strip
    group = iota((size, TILE), 1) // size
    return tuple(
        jnp.concatenate(
            [part * jnp.where(group == q, 1.0, 0.0).astype(BF16) for q in range(TILE // size)], axis=0
        )
        for part in strip
    )


def below(corner, first, second, size):
    inner = mm3(split(corner), spread(split(first), size))
    return mm3(split(second), spread(split(inner), size))


def widen(tiles):
    return [jnp.concatenate(tiles[t : t + 2], axis=1) for t in range(0, len(tiles), 2)]


def narrow(strips):
    return [w[:, h : h + 128] for w in strips for h in (0, 128)]


def small_tiles(diag):
    return [diag[t, h] for t in range(diag.shape[0]) for h in range(2)]


def invert_bases(diag):
    small = small_tiles(diag)
    group = iota((BASE, 128), 1) // BASE
    strips = []
    for tile in small:
        strip = tile[:BASE]
        for q in range(1, 128 // BASE):
            strip = jnp.where(group == q, tile[q * BASE : (q + 1) * BASE], strip)
        strips.append(strip)
    base = invert_base(jnp.concatenate(strips, axis=1))
    return [base[:, t : t + 128] for t in range(0, base.shape[1], 128)]


def invert_small(diag, tiles):
    small = small_tiles(diag)
    size = BASE
    while size < 128:
        group = iota((size, 128), 1) // size
        even = group % 2 == 0
        corners = []
        for tile in small:
            corner = tile[size : 2 * size]
            for q in range(1, 128 // (2 * size)):
                at = (2 * q + 1) * size
                corner = jnp.where(group == 2 * q, tile[at : at + size], corner)
            corners.append(corner)

        def evens(x):
            return [jnp.where(even, x[t], pltpu.roll(x[t + 1], size, 1)) for t in range(0, len(x), 2)]

        def odds(x):
            return [jnp.where(even, pltpu.roll(x[t], 128 - size, 1), x[t + 1]) for t in range(0, len(x), 2)]

        left = narrow(
            [
                below(c, f, g, size)
                for c, f, g in zip(widen(evens(corners)), widen(evens(tiles)), widen(odds(tiles)))
            ]
        )
        merged = []
        for t, tile in enumerate(tiles):
            x = left[t // 2] if t % 2 == 0 else pltpu.roll(left[t // 2], 128 - size, 1)
            merged.append(
                jnp.concatenate([jnp.where(even, tile, 0.0), jnp.where(even, -x, tile)], axis=0)
            )
        tiles = merged
        size *= 2
    return tiles


def invert_tiles(diag, tiles):
    n_tile = diag.shape[0]
    corners = [diag[t, 2] for t in range(n_tile)]
    left = narrow(
        [below(c, f, g, 128) for c, f, g in zip(widen(corners), widen(tiles[::2]), widen(tiles[1::2]))]
    )
    zero = jnp.zeros((128, 128), F32)
    return [
        jnp.concatenate(
            [
                jnp.concatenate([tiles[2 * t], zero], axis=1),
                jnp.concatenate([-left[t], tiles[2 * t + 1]], axis=1),
            ],
            axis=0,
        )
        for t in range(n_tile)
    ]


def parts_of(device):
    col = SIDE * SIDE
    return (
        lax.div(device, CORES * col),
        lax.rem(lax.div(device, col), CORES),
        lax.rem(lax.div(device, SIDE), SIDE),
        lax.rem(device, SIDE),
    )


def joined(y, core, x, z):
    return ((y * CORES + core) * SIDE + x) * SIDE + z


SIZES = (SIDE, CORES, SIDE, SIDE)


def steps_of(offset):
    return (
        offset // (CORES * SIDE * SIDE),
        offset // (SIDE * SIDE) % CORES,
        offset // SIDE % SIDE,
        offset % SIDE,
    )


def opposite(offset):
    return joined(*((n - d) % n for n, d in zip(SIZES, steps_of(offset))))


def hops(offset):
    y, core, x, z = steps_of(offset)
    return sum(min(d, SIDE - d) for d in (y, x, z)) + 0.5 * core


def kernel(
    panel_hbm, factor_hbm, rows_hbm, target_hbm, out_ref,
    panel, rows, diag, sub, off, vh, vl, oh, ol, fwd, place, send0, recv0, send1, recv1, target_ref, result,
    load_sem, send_sem, recv_sem,
):
    n_holders = lax.axis_size("row") * lax.axis_size("col")
    me = lax.axis_index("row") * lax.axis_size("col") + lax.axis_index("col")
    here = parts_of(me)
    n_big = off.shape[0]
    n_tile = diag.shape[0]
    owned = result.shape[0]
    sends, recvs = (send0, send1), (recv0, recv1)
    pairs = [(1, 0), (2, 0), (2, 1)]
    offsets = sorted(range(1, n_holders), key=lambda o: -hops(o))
    ahead = [[lax.rem(c + d, n) for d in range(n)] for c, n in zip(here, SIZES)]
    rows_ahead = [joined(y, core, 0, 0) for y in ahead[0] for core in ahead[1]]
    cols_ahead = [joined(0, 0, x, z) for x in ahead[2] for z in ahead[3]]

    def device_at(o):
        return rows_ahead[o // (SIDE * SIDE)] + cols_ahead[o % (SIDE * SIDE)]

    loads = []

    def load(src, dst):
        cp = pltpu.make_async_copy(src, dst, load_sem.at[len(loads)])
        cp.start()
        loads.append(cp)

    def factor_at(r, c, size):
        return factor_hbm.at[pl.ds(r * size, size), pl.ds(c * size, size)]

    load(target_hbm, target_ref)
    for t in range(n_tile):
        load(factor_at(2 * t, 2 * t, 128), diag.at[t, 0])
        load(factor_at(2 * t + 1, 2 * t + 1, 128), diag.at[t, 1])
    for t in range(n_tile):
        load(factor_at(2 * t + 1, 2 * t, 128), diag.at[t, 2])
    for t in range(n_big):
        load(factor_at(2 * t + 1, 2 * t, TILE), sub.at[t])
    for p, (i, j) in enumerate(pairs):
        load(factor_at(i, j, BIG), off.at[p])
    load(panel_hbm, panel)
    load(rows_hbm, rows)

    with jax.named_scope("greet"):
        barrier = pltpu.get_barrier_semaphore()
        for o in offsets:
            pl.semaphore_signal(barrier, inc=1, device_id=device_at(o), device_id_type=LOGICAL)

    first, second = 2 * n_tile + 1, 3 * n_tile + n_big + 1
    for cp in loads[:first]:
        cp.wait()
    with jax.named_scope("place"):
        sent = target_ref.shape[1]
        target = jnp.broadcast_to(target_ref[...], (8, sent))
        holder = target // owned
        within = target - holder * owned
        lane = iota((8, sent), 1)
        rank = jnp.zeros((8, sent), I32)
        for d in range(1, SLOTS):
            same = (pltpu.roll(holder, d, 1) == holder) & (lane >= d)
            rank = rank + jnp.where(same, 1, 0)
        away = joined(*(lax.rem(h - c + n, n) for h, c, n in zip(parts_of(holder), here, SIZES)))
        position = (away * SLOTS + rank)[:1]
        slots = n_holders * SLOTS
        placed = jnp.where(iota((slots, sent), 0) == position, 1.0, 0.0).astype(BF16)
        place[...] = placed
        described = jnp.concatenate(
            [jnp.broadcast_to(within[:1].astype(F32), (128, sent)), jnp.ones((128, sent), F32)], axis=0
        ).astype(BF16)
        found = mm_nt(placed, described)
        index = found[:, :128] + EMPTY * (1.0 - found[:, 128:])
        send0[:, 2 * SLOTS :] = index.reshape(n_holders, SLOTS, 128).astype(BF16)
    with jax.named_scope("small"):
        small = invert_small(diag, invert_bases(diag))
    for cp in loads[first:second]:
        cp.wait()
    with jax.named_scope("merge"):
        inverse = invert_tiles(diag, small)
        for b in range(n_big):
            left = split(below(sub[b], inverse[2 * b], inverse[2 * b + 1], TILE))
            top, bottom = split(inverse[2 * b]), split(inverse[2 * b + 1])
            for ref, i in ((vh, 0), (vl, 1)):
                ref[b, 0] = top[i]
                ref[b, 1] = left[i]
                ref[b, 2] = bottom[i]
    for cp in loads[second:]:
        cp.wait()
    with jax.named_scope("split"):
        for p in range(len(pairs)):
            oh[p], ol[p] = split(off[p])
    def dispatch(ch):
        for o in offsets:
            pltpu.make_async_remote_copy(
                src_ref=sends[ch].at[o],
                dst_ref=recvs[ch].at[opposite(o)],
                send_sem=send_sem.at[ch],
                recv_sem=recv_sem.at[ch],
                device_id=device_at(o),
                device_id_type=LOGICAL,
            ).start()
        recvs[ch][0] = sends[ch][0]

    others = pl.ds(1, n_holders - 1)

    def arrived(ch):
        pltpu.make_async_copy(sends[ch].at[others], recvs[ch].at[others], recv_sem.at[ch]).wait()

    def left_device(ch):
        pltpu.make_async_copy(sends[ch].at[others], recvs[ch].at[others], send_sem.at[ch]).wait()

    def inv(b, part):
        return (vh[b, part], vl[b, part])

    def halves(x, axis):
        if axis == 0:
            return [tuple(y[:TILE] for y in x), tuple(y[TILE:] for y in x)]
        return [tuple(y[:, :TILE] for y in x), tuple(y[:, TILE:] for y in x)]

    n_chunk = len(sends)
    for ch in range(n_chunk):
        with jax.named_scope("fwd"):
            cols = slice(ch * CHUNK, (ch + 1) * CHUNK)
            rhs = [panel[b * BIG : (b + 1) * BIG, cols].astype(F32) for b in range(n_big)]
            for b in range(n_big):
                r = halves(split(rhs[b]), 0)
                upper = mm3(inv(b, 0), r[0])
                lower = mm3(inv(b, 2), r[1]) - mm3(inv(b, 1), r[0])
                f = jnp.concatenate([upper, lower], axis=0)
                fwd[:, b * BIG : (b + 1) * BIG] = f.T
                fs = halves(split(f), 0)
                for p, (i, j) in enumerate(pairs):
                    if j == b:
                        o = halves((oh[p], ol[p]), 1)
                        rhs[i] = (rhs[i] - mm3(o[0], fs[0])) - mm3(o[1], fs[1])
        with jax.named_scope("bwd"):
            partial = []
            for b in reversed(range(n_big)):
                q = halves(split(fwd[:, b * BIG : (b + 1) * BIG]), 1)
                first = mm3(q[0], inv(b, 0)) - mm3(q[1], inv(b, 1))
                second = mm3(q[1], inv(b, 2))
                x = jnp.concatenate([first, second], axis=1)
                xs = halves(split(x), 1)
                for p, (i, j) in reversed(list(enumerate(pairs))):
                    if i == b:
                        at = slice(j * BIG, (j + 1) * BIG)
                        o = halves((oh[p], ol[p]), 0)
                        fwd[:, at] = (fwd[:, at] - mm3(xs[0], o[0])) - mm3(xs[1], o[1])
                at = b * BIG
                if b:
                    partial.append(mm_nt(rows[:, at : at + BIG], jnp.concatenate([-xs[0][0], -xs[1][0]], axis=1)))
                else:
                    update = mm_nt(rows[:, :TILE], xs[0][0]) - mm_nt(rows[:, TILE:BIG], -xs[1][0])
            for other in partial:
                update = update - other
            update = update.astype(BF16)
        with jax.named_scope("pack"):
            step = n_holders // GROUPS
            for g in range(GROUPS):
                some = slice(g * step, (g + 1) * step)
                packed = mm(place[g * step * SLOTS : (g + 1) * step * SLOTS], update).reshape(step, SLOTS, CHUNK)
                packed = jnp.concatenate([packed[:, :, :128], packed[:, :, 128:]], axis=1).astype(BF16)
                sends[ch][some, : 2 * SLOTS] = packed
        with jax.named_scope("send"):
            if ch == 0:
                pl.semaphore_wait(barrier, n_holders - 1)
            dispatch(ch)

    stores = []
    for ch in range(n_chunk):
        with jax.named_scope("wait"):
            arrived(ch)
        with jax.named_scope("final"):
            if ch == 0:
                pick0 = jnp.where(iota((8, 128), 1) == 0, 1.0, 0.0).astype(BF16)
                named = mm_nt(pick0, recv0[:, 2 * SLOTS :].astype(F32).reshape(slots, 128).astype(BF16))[:1]
                gather = jnp.where(iota((owned, slots), 0).astype(F32) == named, 1.0, 0.0).astype(BF16)
            got = recvs[ch][:, : 2 * SLOTS].astype(F32)
            got = jnp.concatenate(
                [got[:, :SLOTS].reshape(slots, 128), got[:, SLOTS:].reshape(slots, 128)], axis=1
            )
            cols = pl.ds(ch * CHUNK, CHUNK)
            result[:, cols] = mm(gather, got.astype(BF16))
        store = pltpu.make_async_copy(result.at[:, cols], out_ref.at[:, cols], load_sem.at[ch])
        store.start()
        stores.append(store)
    for ch in range(n_chunk):
        left_device(ch)
        stores[ch].wait()


def local(coupling_panel, interior_factor, border_rows, target_rows, border_block):
    panel, factor, rows = coupling_panel[0], interior_factor[0], border_rows[0]
    n, width = panel.shape
    holders = lax.axis_size("row") * lax.axis_size("col")
    n_tile, n_big, n_chunk = n // TILE, n // BIG, width // CHUNK
    pairs = n_big * (n_big - 1) // 2
    hbm = pl.BlockSpec(memory_space=pl.ANY)
    assembled = pl.pallas_call(
        kernel,
        out_shape=jax.ShapeDtypeStruct(border_block.shape, F32),
        in_specs=[hbm] * 4,
        out_specs=hbm,
        scratch_shapes=[
            pltpu.VMEM(panel.shape, BF16),
            pltpu.VMEM(rows.shape, BF16),
            pltpu.VMEM((n_tile, 3, 128, 128), F32),
            pltpu.VMEM((n_big, TILE, TILE), F32),
            pltpu.VMEM((pairs, BIG, BIG), F32),
            pltpu.VMEM((n_big, 3, TILE, TILE), BF16),
            pltpu.VMEM((n_big, 3, TILE, TILE), BF16),
            pltpu.VMEM((pairs, BIG, BIG), BF16),
            pltpu.VMEM((pairs, BIG, BIG), BF16),
            pltpu.VMEM((CHUNK, n), F32),
            pltpu.VMEM((holders * SLOTS, target_rows.shape[1]), BF16),
            pltpu.VMEM((holders, 3 * SLOTS, 128), BF16),
            pltpu.VMEM((holders, 3 * SLOTS, 128), BF16),
            pltpu.VMEM((holders, 2 * SLOTS, 128), BF16),
            pltpu.VMEM((holders, 2 * SLOTS, 128), BF16),
            pltpu.VMEM(target_rows.shape, I32),
            pltpu.VMEM(border_block.shape, F32),
            pltpu.SemaphoreType.DMA((3 * n_tile + n_big + pairs + 3,)),
            pltpu.SemaphoreType.DMA((n_chunk,)),
            pltpu.SemaphoreType.DMA((n_chunk,)),
        ],
        compiler_params=pltpu.CompilerParams(
            collective_id=0, has_side_effects=True, vmem_limit_bytes=53 * 1024 * 1024
        ),
        name="schur_panel",
    )(panel, factor, rows, target_rows)
    return border_block - assembled


def solution(mesh):
    placed = (
        P("row", None, None),
        P("row", None, None),
        P("row", "col", None),
        P("row", "col"),
        P(("row", "col"), None),
    )
    return jax.shard_map(
        local, mesh=mesh, in_specs=placed, out_specs=P(("row", "col"), None), check_vma=False
    )
```

```python
import jax
import jax.numpy as jnp
from jax import lax
from jax.experimental import pallas as pl
from jax.experimental.pallas import tpu as pltpu
from jax.sharding import PartitionSpec as P

F32, BF16, I32 = jnp.float32, jnp.bfloat16, jnp.int32
BASE = 16
TILE = 256
BIG = 512
CHUNK = 256
SLOTS = 8
GROUPS = 2
SIDE = 4
CORES = 2
LOGICAL = pl.DeviceIdType.LOGICAL
EMPTY = -512.0


def iota(shape, axis):
    return lax.broadcasted_iota(I32, shape, axis)


def split(x):
    hi = x.astype(BF16)
    return hi, (x - hi.astype(F32)).astype(BF16)


def mm(a, b):
    return jnp.dot(a, b, preferred_element_type=F32)


def mm_nt(a, b):
    return lax.dot_general(a, b, (((1,), (1,)), ((), ())), preferred_element_type=F32)


def mm3(a, b):
    return mm(a[0], b[0]) + (mm(a[0], b[1]) + mm(a[1], b[0]))


def invert_base(strip):
    rows, width = strip.shape
    lane = iota((rows, width), 1)
    row = iota((rows, width), 0)
    within = lane % BASE
    start = lane - within
    tiles = range(0, width, 128)
    local = (lane - within)[:, :128] % 128

    def pick(x, index):
        return jnp.concatenate(
            [jnp.take_along_axis(x[:, t : t + 128], index[: x.shape[0]], axis=1) for t in tiles], axis=1
        )

    recip = 1.0 / pick(strip, local + row[:, :128])
    scaled = jnp.where(within < row, strip * recip, 0.0)
    inverse = jnp.where(within == row, recip, 0.0)
    for k in range(rows - 1):
        first = (k + 1) // 8 * 8
        factor = pick(scaled[first:], local + k)
        update = inverse[first:] - factor * inverse[k : k + 1]
        inverse = update if first == 0 else jnp.concatenate([inverse[:first], update], axis=0)
    return inverse


def stacked(a, b):
    rows = a[0].shape[0]
    both = mm(jnp.concatenate(a, axis=0), b[0])
    return both[:rows] + (both[rows:] + mm(a[0], b[1]))


def spread(strip, size):
    width = strip[0].shape[1]
    if size == width:
        return strip
    group = iota((size, width), 1) // size
    return tuple(
        jnp.concatenate(
            [part * jnp.where(group == q, 1.0, 0.0).astype(BF16) for q in range(width // size)], axis=0
        )
        for part in strip
    )


def below(corner, first, second, size):
    inner = stacked(split(corner), spread(split(first), size))
    return stacked(split(second), spread(split(inner), size))


def small_tiles(diag):
    return [diag[t, h] for t in range(diag.shape[0]) for h in range(2)]


def invert_bases(diag):
    small = small_tiles(diag)
    group = iota((BASE, 128), 1) // BASE
    strips = []
    for tile in small:
        strip = tile[:BASE]
        for q in range(1, 128 // BASE):
            strip = jnp.where(group == q, tile[q * BASE : (q + 1) * BASE], strip)
        strips.append(strip)
    base = invert_base(jnp.concatenate(strips, axis=1))
    return [base[:, t : t + 128] for t in range(0, base.shape[1], 128)]


def invert_small(diag, tiles):
    small = small_tiles(diag)
    size = BASE
    while size < 128:
        group = iota((size, 128), 1) // size
        even = group % 2 == 0
        corners = []
        for tile in small:
            corner = tile[size : 2 * size]
            for q in range(1, 128 // (2 * size)):
                at = (2 * q + 1) * size
                corner = jnp.where(group == 2 * q, tile[at : at + size], corner)
            corners.append(corner)

        def evens(x):
            return [jnp.where(even, x[t], pltpu.roll(x[t + 1], size, 1)) for t in range(0, len(x), 2)]

        def odds(x):
            return [jnp.where(even, pltpu.roll(x[t], 128 - size, 1), x[t + 1]) for t in range(0, len(x), 2)]

        left = [below(c, f, g, size) for c, f, g in zip(evens(corners), evens(tiles), odds(tiles))]
        merged = []
        for t, tile in enumerate(tiles):
            x = left[t // 2] if t % 2 == 0 else pltpu.roll(left[t // 2], 128 - size, 1)
            merged.append(
                jnp.concatenate([jnp.where(even, tile, 0.0), jnp.where(even, -x, tile)], axis=0)
            )
        tiles = merged
        size *= 2
    return tiles


def invert_tiles(diag, tiles):
    n_tile = diag.shape[0]
    left = [below(diag[t, 2], tiles[2 * t], tiles[2 * t + 1], 128) for t in range(n_tile)]
    zero = jnp.zeros((128, 128), F32)
    return [
        jnp.concatenate(
            [
                jnp.concatenate([tiles[2 * t], zero], axis=1),
                jnp.concatenate([-left[t], tiles[2 * t + 1]], axis=1),
            ],
            axis=0,
        )
        for t in range(n_tile)
    ]


def parts_of(device):
    col = SIDE * SIDE
    return (
        lax.div(device, CORES * col),
        lax.rem(lax.div(device, col), CORES),
        lax.rem(lax.div(device, SIDE), SIDE),
        lax.rem(device, SIDE),
    )


def joined(y, core, x, z):
    return ((y * CORES + core) * SIDE + x) * SIDE + z


SIZES = (SIDE, CORES, SIDE, SIDE)


def steps_of(offset):
    return (
        offset // (CORES * SIDE * SIDE),
        offset // (SIDE * SIDE) % CORES,
        offset // SIDE % SIDE,
        offset % SIDE,
    )


def opposite(offset):
    return joined(*((n - d) % n for n, d in zip(SIZES, steps_of(offset))))


def hops(offset):
    y, core, x, z = steps_of(offset)
    return sum(min(d, SIDE - d) for d in (y, x, z)) + 0.5 * core


def send_order(n):
    classes = {}
    for o in sorted(range(1, n), key=lambda o: -hops(o)):
        y, core, x, z = steps_of(o)
        moved = ("x", x) if x else ("y", y) if y else ("z", z)
        classes.setdefault(moved, []).append(o)
    placed = [((i + 0.5) / len(c), -len(c), o) for c in classes.values() for i, o in enumerate(c)]
    return [o for _, _, o in sorted(placed)]


def kernel(
    panel_hbm, factor_hbm, rows_hbm, target_hbm, out_ref,
    panel, rows, diag, sub, off, vh, vl, oh, ol, fwd, place, send0, recv0, send1, recv1, target_ref, result,
    load_sem, send_sem, recv_sem,
):
    n_holders = lax.axis_size("row") * lax.axis_size("col")
    me = lax.axis_index("row") * lax.axis_size("col") + lax.axis_index("col")
    here = parts_of(me)
    n_big = off.shape[0]
    n_tile = diag.shape[0]
    owned = result.shape[0]
    sends, recvs = (send0, send1), (recv0, recv1)
    pairs = [(1, 0), (2, 0), (2, 1)]
    offsets = send_order(n_holders)
    ahead = [[lax.rem(c + d, n) for d in range(n)] for c, n in zip(here, SIZES)]
    rows_ahead = [joined(y, core, 0, 0) for y in ahead[0] for core in ahead[1]]
    cols_ahead = [joined(0, 0, x, z) for x in ahead[2] for z in ahead[3]]

    def device_at(o):
        return rows_ahead[o // (SIDE * SIDE)] + cols_ahead[o % (SIDE * SIDE)]

    loads = []

    def load(src, dst):
        cp = pltpu.make_async_copy(src, dst, load_sem.at[len(loads)])
        cp.start()
        loads.append(cp)

    def factor_at(r, c, size):
        return factor_hbm.at[pl.ds(r * size, size), pl.ds(c * size, size)]

    load(target_hbm, target_ref)
    for t in range(n_tile):
        load(factor_at(2 * t, 2 * t, 128), diag.at[t, 0])
        load(factor_at(2 * t + 1, 2 * t + 1, 128), diag.at[t, 1])
    for t in range(n_tile):
        load(factor_at(2 * t + 1, 2 * t, 128), diag.at[t, 2])
    for t in range(n_big):
        load(factor_at(2 * t + 1, 2 * t, TILE), sub.at[t])
    for p, (i, j) in enumerate(pairs):
        load(factor_at(i, j, BIG), off.at[p])
    load(panel_hbm, panel)
    load(rows_hbm, rows)

    with jax.named_scope("greet"):
        barrier = pltpu.get_barrier_semaphore()
        for o in offsets:
            pl.semaphore_signal(barrier, inc=1, device_id=device_at(o), device_id_type=LOGICAL)

    first, second = 2 * n_tile + 1, 3 * n_tile + n_big + 1
    for cp in loads[:first]:
        cp.wait()
    with jax.named_scope("place"):
        sent = target_ref.shape[1]
        target = jnp.broadcast_to(target_ref[...], (8, sent))
        holder = target // owned
        within = target - holder * owned
        lane = iota((8, sent), 1)
        rank = jnp.zeros((8, sent), I32)
        for d in range(1, SLOTS):
            same = (pltpu.roll(holder, d, 1) == holder) & (lane >= d)
            rank = rank + jnp.where(same, 1, 0)
        away = joined(*(lax.rem(h - c + n, n) for h, c, n in zip(parts_of(holder), here, SIZES)))
        position = (away * SLOTS + rank)[:1]
        slots = n_holders * SLOTS
        placed = jnp.where(iota((slots, sent), 0) == position, 1.0, 0.0).astype(BF16)
        place[...] = placed
        described = jnp.concatenate(
            [jnp.broadcast_to(within[:1].astype(F32), (128, sent)), jnp.ones((128, sent), F32)], axis=0
        ).astype(BF16)
        found = mm_nt(placed, described)
        index = found[:, :128] + EMPTY * (1.0 - found[:, 128:])
        send0[:, 2 * SLOTS :] = index.reshape(n_holders, SLOTS, 128).astype(BF16)
    with jax.named_scope("small"):
        small = invert_small(diag, invert_bases(diag))
    for cp in loads[first:second]:
        cp.wait()
    with jax.named_scope("merge"):
        inverse = invert_tiles(diag, small)
        for b in range(n_big):
            left = split(below(sub[b], inverse[2 * b], inverse[2 * b + 1], TILE))
            top, bottom = split(inverse[2 * b]), split(inverse[2 * b + 1])
            for ref, i in ((vh, 0), (vl, 1)):
                ref[b, 0] = top[i]
                ref[b, 1] = left[i]
                ref[b, 2] = bottom[i]
    for cp in loads[second:]:
        cp.wait()
    with jax.named_scope("split"):
        for p in range(len(pairs)):
            oh[p], ol[p] = split(off[p])
    def dispatch(ch):
        for o in offsets:
            pltpu.make_async_remote_copy(
                src_ref=sends[ch].at[o],
                dst_ref=recvs[ch].at[opposite(o)],
                send_sem=send_sem.at[ch],
                recv_sem=recv_sem.at[ch],
                device_id=device_at(o),
                device_id_type=LOGICAL,
            ).start()
        recvs[ch][0] = sends[ch][0]

    others = pl.ds(1, n_holders - 1)

    def arrived(ch):
        pltpu.make_async_copy(sends[ch].at[others], recvs[ch].at[others], recv_sem.at[ch]).wait()

    def left_device(ch):
        pltpu.make_async_copy(sends[ch].at[others], recvs[ch].at[others], send_sem.at[ch]).wait()

    def inv(b, part):
        return (vh[b, part], vl[b, part])

    def halves(x, axis):
        if axis == 0:
            return [tuple(y[:TILE] for y in x), tuple(y[TILE:] for y in x)]
        return [tuple(y[:, :TILE] for y in x), tuple(y[:, TILE:] for y in x)]

    n_chunk = len(sends)
    for ch in range(n_chunk):
        with jax.named_scope("fwd"):
            cols = slice(ch * CHUNK, (ch + 1) * CHUNK)
            rhs = [panel[b * BIG : (b + 1) * BIG, cols].astype(F32) for b in range(n_big)]
            for b in range(n_big):
                r = halves(split(rhs[b]), 0)
                upper = mm3(inv(b, 0), r[0])
                lower = mm3(inv(b, 2), r[1]) - mm3(inv(b, 1), r[0])
                f = jnp.concatenate([upper, lower], axis=0)
                fwd[:, b * BIG : (b + 1) * BIG] = f.T
                fs = halves(split(f), 0)
                for p, (i, j) in enumerate(pairs):
                    if j == b:
                        o = halves((oh[p], ol[p]), 1)
                        rhs[i] = (rhs[i] - mm3(o[0], fs[0])) - mm3(o[1], fs[1])
        with jax.named_scope("bwd"):
            partial = []
            for b in reversed(range(n_big)):
                q = halves(split(fwd[:, b * BIG : (b + 1) * BIG]), 1)
                first = mm3(q[0], inv(b, 0)) - mm3(q[1], inv(b, 1))
                second = mm3(q[1], inv(b, 2))
                x = jnp.concatenate([first, second], axis=1)
                xs = halves(split(x), 1)
                for p, (i, j) in reversed(list(enumerate(pairs))):
                    if i == b:
                        at = slice(j * BIG, (j + 1) * BIG)
                        o = halves((oh[p], ol[p]), 0)
                        fwd[:, at] = (fwd[:, at] - mm3(xs[0], o[0])) - mm3(xs[1], o[1])
                at = b * BIG
                if b:
                    partial.append(mm_nt(rows[:, at : at + BIG], jnp.concatenate([-xs[0][0], -xs[1][0]], axis=1)))
                else:
                    update = mm_nt(rows[:, :TILE], xs[0][0]) - mm_nt(rows[:, TILE:BIG], -xs[1][0])
            for other in partial:
                update = update - other
            update = update.astype(BF16)
        with jax.named_scope("pack"):
            step = n_holders // GROUPS
            for g in range(GROUPS):
                some = slice(g * step, (g + 1) * step)
                packed = mm(place[g * step * SLOTS : (g + 1) * step * SLOTS], update).reshape(step, SLOTS, CHUNK)
                packed = jnp.concatenate([packed[:, :, :128], packed[:, :, 128:]], axis=1).astype(BF16)
                sends[ch][some, : 2 * SLOTS] = packed
        with jax.named_scope("send"):
            if ch == 0:
                pl.semaphore_wait(barrier, n_holders - 1)
            dispatch(ch)

    stores = []
    for ch in range(n_chunk):
        with jax.named_scope("wait"):
            arrived(ch)
        with jax.named_scope("final"):
            if ch == 0:
                pick0 = jnp.where(iota((8, 128), 1) == 0, 1.0, 0.0).astype(BF16)
                named = mm_nt(pick0, recv0[:, 2 * SLOTS :].astype(F32).reshape(slots, 128).astype(BF16))[:1]
                gather = jnp.where(iota((owned, slots), 0).astype(F32) == named, 1.0, 0.0).astype(BF16)
            got = recvs[ch][:, : 2 * SLOTS].astype(F32)
            got = jnp.concatenate(
                [got[:, :SLOTS].reshape(slots, 128), got[:, SLOTS:].reshape(slots, 128)], axis=1
            )
            cols = pl.ds(ch * CHUNK, CHUNK)
            result[:, cols] = mm(gather, got.astype(BF16))
        store = pltpu.make_async_copy(result.at[:, cols], out_ref.at[:, cols], load_sem.at[ch])
        store.start()
        stores.append(store)
    for ch in range(n_chunk):
        left_device(ch)
        stores[ch].wait()


def local(coupling_panel, interior_factor, border_rows, target_rows, border_block):
    panel, factor, rows = coupling_panel[0], interior_factor[0], border_rows[0]
    n, width = panel.shape
    holders = lax.axis_size("row") * lax.axis_size("col")
    n_tile, n_big, n_chunk = n // TILE, n // BIG, width // CHUNK
    pairs = n_big * (n_big - 1) // 2
    hbm = pl.BlockSpec(memory_space=pl.ANY)
    assembled = pl.pallas_call(
        kernel,
        out_shape=jax.ShapeDtypeStruct(border_block.shape, F32),
        in_specs=[hbm] * 4,
        out_specs=hbm,
        scratch_shapes=[
            pltpu.VMEM(panel.shape, BF16),
            pltpu.VMEM(rows.shape, BF16),
            pltpu.VMEM((n_tile, 3, 128, 128), F32),
            pltpu.VMEM((n_big, TILE, TILE), F32),
            pltpu.VMEM((pairs, BIG, BIG), F32),
            pltpu.VMEM((n_big, 3, TILE, TILE), BF16),
            pltpu.VMEM((n_big, 3, TILE, TILE), BF16),
            pltpu.VMEM((pairs, BIG, BIG), BF16),
            pltpu.VMEM((pairs, BIG, BIG), BF16),
            pltpu.VMEM((CHUNK, n), F32),
            pltpu.VMEM((holders * SLOTS, target_rows.shape[1]), BF16),
            pltpu.VMEM((holders, 3 * SLOTS, 128), BF16),
            pltpu.VMEM((holders, 3 * SLOTS, 128), BF16),
            pltpu.VMEM((holders, 2 * SLOTS, 128), BF16),
            pltpu.VMEM((holders, 2 * SLOTS, 128), BF16),
            pltpu.VMEM(target_rows.shape, I32),
            pltpu.VMEM(border_block.shape, F32),
            pltpu.SemaphoreType.DMA((3 * n_tile + n_big + pairs + 3,)),
            pltpu.SemaphoreType.DMA((n_chunk,)),
            pltpu.SemaphoreType.DMA((n_chunk,)),
        ],
        compiler_params=pltpu.CompilerParams(
            collective_id=0, has_side_effects=True, vmem_limit_bytes=53 * 1024 * 1024
        ),
        name="schur_panel",
    )(panel, factor, rows, target_rows)
    return border_block - assembled


def solution(mesh):
    placed = (
        P("row", None, None),
        P("row", None, None),
        P("row", "col", None),
        P("row", "col"),
        P(("row", "col"), None),
    )
    return jax.shard_map(
        local, mesh=mesh, in_specs=placed, out_specs=P(("row", "col"), None), check_vma=False
    )
```

```python
import jax
import jax.numpy as jnp
from jax import lax
from jax.experimental import pallas as pl
from jax.experimental.pallas import tpu as pltpu
from jax.sharding import PartitionSpec as P

F32, BF16, I32 = jnp.float32, jnp.bfloat16, jnp.int32
BASE = 16
TILE = 256
BIG = 512
CHUNK = 256
SLOTS = 8
GROUPS = 2
SIDE = 4
CORES = 2
LOGICAL = pl.DeviceIdType.LOGICAL
EMPTY = -512.0


def iota(shape, axis):
    return lax.broadcasted_iota(I32, shape, axis)


def split(x):
    hi = x.astype(BF16)
    return hi, (x - hi.astype(F32)).astype(BF16)


def mm(a, b):
    return jnp.dot(a, b, preferred_element_type=F32)


def mm_nt(a, b):
    return lax.dot_general(a, b, (((1,), (1,)), ((), ())), preferred_element_type=F32)


def mm3(a, b):
    return mm(a[0], b[0]) + (mm(a[0], b[1]) + mm(a[1], b[0]))


def invert_base(strip):
    rows, width = strip.shape
    lane = iota((rows, width), 1)
    row = iota((rows, width), 0)
    within = lane % BASE
    start = lane - within
    tiles = range(0, width, 128)
    local = (lane - within)[:, :128] % 128

    def pick(x, index):
        return jnp.concatenate(
            [jnp.take_along_axis(x[:, t : t + 128], index[: x.shape[0]], axis=1) for t in tiles], axis=1
        )

    recip = 1.0 / pick(strip, local + row[:, :128])
    scaled = jnp.where(within < row, strip * recip, 0.0)
    inverse = jnp.where(within == row, recip, 0.0)
    for k in range(rows - 1):
        first = (k + 1) // 8 * 8
        factor = pick(scaled[first:], local + k)
        update = inverse[first:] - factor * inverse[k : k + 1]
        inverse = update if first == 0 else jnp.concatenate([inverse[:first], update], axis=0)
    return inverse


def stacked(a, b):
    rows = a[0].shape[0]
    both = mm(jnp.concatenate(a, axis=0), b[0])
    return both[:rows] + (both[rows:] + mm(a[0], b[1]))


def spread(strip, size):
    width = strip[0].shape[1]
    if size == width:
        return strip
    group = iota((size, width), 1) // size
    return tuple(
        jnp.concatenate(
            [part * jnp.where(group == q, 1.0, 0.0).astype(BF16) for q in range(width // size)], axis=0
        )
        for part in strip
    )


def below(corner, first, second, size):
    inner = stacked(split(corner), spread(split(first), size))
    return stacked(split(second), spread(split(inner), size))


def small_tiles(diag):
    return [diag[t, h] for t in range(diag.shape[0]) for h in range(2)]


def invert_bases(diag):
    small = small_tiles(diag)
    group = iota((BASE, 128), 1) // BASE
    strips = []
    for tile in small:
        strip = tile[:BASE]
        for q in range(1, 128 // BASE):
            strip = jnp.where(group == q, tile[q * BASE : (q + 1) * BASE], strip)
        strips.append(strip)
    base = invert_base(jnp.concatenate(strips, axis=1))
    return [base[:, t : t + 128] for t in range(0, base.shape[1], 128)]


def invert_small(diag, tiles, between):
    small = small_tiles(diag)
    size = BASE
    while size < 128:
        between()
        group = iota((size, 128), 1) // size
        even = group % 2 == 0
        corners = []
        for tile in small:
            corner = tile[size : 2 * size]
            for q in range(1, 128 // (2 * size)):
                at = (2 * q + 1) * size
                corner = jnp.where(group == 2 * q, tile[at : at + size], corner)
            corners.append(corner)

        def evens(x):
            return [jnp.where(even, x[t], pltpu.roll(x[t + 1], size, 1)) for t in range(0, len(x), 2)]

        def odds(x):
            return [jnp.where(even, pltpu.roll(x[t], 128 - size, 1), x[t + 1]) for t in range(0, len(x), 2)]

        left = [below(c, f, g, size) for c, f, g in zip(evens(corners), evens(tiles), odds(tiles))]
        merged = []
        for t, tile in enumerate(tiles):
            x = left[t // 2] if t % 2 == 0 else pltpu.roll(left[t // 2], 128 - size, 1)
            merged.append(
                jnp.concatenate([jnp.where(even, tile, 0.0), jnp.where(even, -x, tile)], axis=0)
            )
        tiles = merged
        size *= 2
    return tiles


def invert_tiles(diag, tiles):
    n_tile = diag.shape[0]
    left = [below(diag[t, 2], tiles[2 * t], tiles[2 * t + 1], 128) for t in range(n_tile)]
    zero = jnp.zeros((128, 128), F32)
    return [
        jnp.concatenate(
            [
                jnp.concatenate([tiles[2 * t], zero], axis=1),
                jnp.concatenate([-left[t], tiles[2 * t + 1]], axis=1),
            ],
            axis=0,
        )
        for t in range(n_tile)
    ]


def parts_of(device):
    col = SIDE * SIDE
    return (
        lax.div(device, CORES * col),
        lax.rem(lax.div(device, col), CORES),
        lax.rem(lax.div(device, SIDE), SIDE),
        lax.rem(device, SIDE),
    )


def joined(y, core, x, z):
    return ((y * CORES + core) * SIDE + x) * SIDE + z


SIZES = (SIDE, CORES, SIDE, SIDE)


def steps_of(offset):
    return (
        offset // (CORES * SIDE * SIDE),
        offset // (SIDE * SIDE) % CORES,
        offset // SIDE % SIDE,
        offset % SIDE,
    )


def opposite(offset):
    return joined(*((n - d) % n for n, d in zip(SIZES, steps_of(offset))))


def hops(offset):
    y, core, x, z = steps_of(offset)
    return sum(min(d, SIDE - d) for d in (y, x, z)) + 0.5 * core


def send_order(n):
    classes = {}
    for o in sorted(range(1, n), key=lambda o: -hops(o)):
        y, core, x, z = steps_of(o)
        moved = ("x", x) if x else ("y", y) if y else ("z", z)
        classes.setdefault(moved, []).append(o)
    placed = [((i + 0.5) / len(c), -len(c), o) for c in classes.values() for i, o in enumerate(c)]
    return [o for _, _, o in sorted(placed)]


def kernel(
    panel_hbm, factor_hbm, rows_hbm, target_hbm, out_ref,
    panel, rows, diag, sub, off, vh, vl, oh, ol, fwd, place, send0, recv0, send1, recv1,
    row_send, row_recv, col_recv, target_ref, result,
    load_sem, send_sem, recv_sem,
):
    n_holders = lax.axis_size("row") * lax.axis_size("col")
    me = lax.axis_index("row") * lax.axis_size("col") + lax.axis_index("col")
    here = parts_of(me)
    n_col = SIDE * SIDE
    n_row = n_holders // n_col
    n_big = off.shape[0]
    n_tile = diag.shape[0]
    owned = result.shape[0]
    sends, recvs = (send0, send1), (recv0, recv1)
    n_chunk = len(sends)
    pairs = [(1, 0), (2, 0), (2, 1)]
    offsets = send_order(n_holders)
    ahead = [[lax.rem(c + d, n) for d in range(n)] for c, n in zip(here, SIZES)]
    rows_ahead = [joined(y, core, 0, 0) for y in ahead[0] for core in ahead[1]]
    cols_ahead = [joined(0, 0, x, z) for x in ahead[2] for z in ahead[3]]

    def device_at(o):
        return rows_ahead[o // (SIDE * SIDE)] + cols_ahead[o % (SIDE * SIDE)]

    loads = []

    def load(src, dst):
        cp = pltpu.make_async_copy(src, dst, load_sem.at[len(loads)])
        cp.start()
        loads.append(cp)

    def factor_at(r, c, size):
        return factor_hbm.at[pl.ds(r * size, size), pl.ds(c * size, size)]

    load(target_hbm, target_ref)
    for t in range(n_tile):
        load(factor_at(2 * t, 2 * t, 128), diag.at[t, 0])
        load(factor_at(2 * t + 1, 2 * t + 1, 128), diag.at[t, 1])
    for t in range(n_tile):
        load(factor_at(2 * t + 1, 2 * t, 128), diag.at[t, 2])
    for t in range(n_big):
        load(factor_at(2 * t + 1, 2 * t, TILE), sub.at[t])
    for p, (i, j) in enumerate(pairs):
        load(factor_at(i, j, BIG), off.at[p])
    load(panel_hbm, panel)
    load(rows_hbm, rows)

    barrier = pltpu.get_barrier_semaphore()

    @pl.when(me != 0)
    def _():
        pl.semaphore_signal(barrier, inc=1, device_id=0, device_id_type=LOGICAL)

    def all_entered():
        @pl.when(me == 0)
        def _():
            pl.semaphore_wait(barrier, n_holders - 1)
            for o in range(1, n_holders):
                pl.semaphore_signal(barrier, inc=1, device_id=o, device_id_type=LOGICAL)

        @pl.when(me != 0)
        def _():
            pl.semaphore_wait(barrier, 1)

    first, second = 2 * n_tile + 1, 3 * n_tile + n_big + 1
    loads[0].wait()
    with jax.named_scope("place"):
        sent = target_ref.shape[1]
        target = jnp.broadcast_to(target_ref[...], (8, sent))
        holder = target // owned
        within = target - holder * owned
        lane = iota((8, sent), 1)
        rank = jnp.zeros((8, sent), I32)
        for d in range(1, SLOTS):
            same = (pltpu.roll(holder, d, 1) == holder) & (lane >= d)
            rank = rank + jnp.where(same, 1, 0)
        away = joined(*(lax.rem(h - c + n, n) for h, c, n in zip(parts_of(holder), here, SIZES)))
        position = (away * SLOTS + rank)[:1]
        slots = n_holders * SLOTS
        placed = jnp.where(iota((slots, sent), 0) == position, 1.0, 0.0).astype(BF16)
        place[...] = placed
        described = jnp.concatenate(
            [jnp.broadcast_to(within[:1].astype(F32), (128, sent)), jnp.ones((128, sent), F32)], axis=0
        ).astype(BF16)
        found = mm_nt(placed, described)
        index = found[:, :128] + EMPTY * (1.0 - found[:, 128:])
        index = index.reshape(n_row, n_col, SLOTS, 128).astype(BF16)
        for c in range(n_col):
            row_send[c] = index[:, c]
    for cp in loads[1:first]:
        cp.wait()
    waiting = loads[first:second]

    def between():
        waiting.pop(0).wait()

    with jax.named_scope("small"):
        small = invert_small(diag, invert_bases(diag), between)
    for cp in waiting:
        cp.wait()
    with jax.named_scope("merge"):
        inverse = invert_tiles(diag, small)
        for b in range(n_big):
            left = split(below(sub[b], inverse[2 * b], inverse[2 * b + 1], TILE))
            top, bottom = split(inverse[2 * b]), split(inverse[2 * b + 1])
            for ref, i in ((vh, 0), (vl, 1)):
                ref[b, 0] = top[i]
                ref[b, 1] = left[i]
                ref[b, 2] = bottom[i]
    for cp in loads[second:]:
        cp.wait()
    def dispatch(ch):
        for o in offsets:
            pltpu.make_async_remote_copy(
                src_ref=sends[ch].at[o],
                dst_ref=recvs[ch].at[opposite(o)],
                send_sem=send_sem.at[ch],
                recv_sem=recv_sem.at[ch],
                device_id=device_at(o),
                device_id_type=LOGICAL,
            ).start()
        recvs[ch][0] = sends[ch][0]

    others = pl.ds(1, n_holders - 1)

    def arrived(ch):
        pltpu.make_async_copy(sends[ch].at[others], recvs[ch].at[others], recv_sem.at[ch]).wait()

    def left_device(ch):
        pltpu.make_async_copy(sends[ch].at[others], recvs[ch].at[others], send_sem.at[ch]).wait()

    def start(src, dst, o, at):
        pltpu.make_async_remote_copy(
            src_ref=src, dst_ref=dst, send_sem=send_sem.at[at], recv_sem=recv_sem.at[at],
            device_id=device_at(o), device_id_type=LOGICAL,
        ).start()

    def index_to_row():
        for o in range(1, n_col):
            start(row_send.at[o], row_recv.at[opposite(o)], o, n_chunk)
        row_recv[0] = row_send[0]

    def index_to_col():
        peers = pl.ds(1, n_col - 1)
        pltpu.make_async_copy(row_send.at[peers], row_recv.at[peers], recv_sem.at[n_chunk]).wait()
        for r in range(1, n_row):
            back = opposite(r * n_col) // n_col
            start(row_recv.at[:, r], col_recv.at[back], r * n_col, n_chunk + 1)
        col_recv[0] = row_recv[:, 0]
        pltpu.make_async_copy(row_send.at[peers], row_recv.at[peers], send_sem.at[n_chunk]).wait()

    def index_done():
        peers = pl.ds(0, n_row - 1)
        for sem in (recv_sem, send_sem):
            pltpu.make_async_copy(row_recv.at[:, peers], row_recv.at[:, peers], sem.at[n_chunk + 1]).wait()

    def inv(b, part):
        return (vh[b, part], vl[b, part])

    def halves(x, axis):
        if axis == 0:
            return [tuple(y[:TILE] for y in x), tuple(y[TILE:] for y in x)]
        return [tuple(y[:, :TILE] for y in x), tuple(y[:, TILE:] for y in x)]

    with jax.named_scope("barwait"):
        all_entered()
        index_to_row()
    with jax.named_scope("split"):
        for p in range(len(pairs)):
            oh[p], ol[p] = split(off[p])
    for ch in range(n_chunk):
        with jax.named_scope("fwd"):
            cols = slice(ch * CHUNK, (ch + 1) * CHUNK)
            rhs = [panel[b * BIG : (b + 1) * BIG, cols].astype(F32) for b in range(n_big)]
            for b in range(n_big):
                r = halves(split(rhs[b]), 0)
                upper = mm3(inv(b, 0), r[0])
                lower = mm3(inv(b, 2), r[1]) - mm3(inv(b, 1), r[0])
                f = jnp.concatenate([upper, lower], axis=0)
                fwd[:, b * BIG : (b + 1) * BIG] = f.T
                fs = halves(split(f), 0)
                for p, (i, j) in enumerate(pairs):
                    if j == b:
                        o = halves((oh[p], ol[p]), 1)
                        rhs[i] = (rhs[i] - mm3(o[0], fs[0])) - mm3(o[1], fs[1])
        if ch == 0:
            with jax.named_scope("idx"):
                index_to_col()
        with jax.named_scope("bwd"):
            partial = []
            for b in reversed(range(n_big)):
                q = halves(split(fwd[:, b * BIG : (b + 1) * BIG]), 1)
                first = mm3(q[0], inv(b, 0)) - mm3(q[1], inv(b, 1))
                second = mm3(q[1], inv(b, 2))
                x = jnp.concatenate([first, second], axis=1)
                xs = halves(split(x), 1)
                for p, (i, j) in reversed(list(enumerate(pairs))):
                    if i == b:
                        at = slice(j * BIG, (j + 1) * BIG)
                        o = halves((oh[p], ol[p]), 0)
                        fwd[:, at] = (fwd[:, at] - mm3(xs[0], o[0])) - mm3(xs[1], o[1])
                at = b * BIG
                if b:
                    partial.append(mm_nt(rows[:, at : at + BIG], jnp.concatenate([-xs[0][0], -xs[1][0]], axis=1)))
                else:
                    update = mm_nt(rows[:, :TILE], xs[0][0]) - mm_nt(rows[:, TILE:BIG], -xs[1][0])
            for other in partial:
                update = update - other
            update = update.astype(BF16)
        with jax.named_scope("pack"):
            step = n_holders // GROUPS
            for g in range(GROUPS):
                some = slice(g * step, (g + 1) * step)
                packed = mm(place[g * step * SLOTS : (g + 1) * step * SLOTS], update).reshape(step, SLOTS, CHUNK)
                packed = jnp.concatenate([packed[:, :, :128], packed[:, :, 128:]], axis=1).astype(BF16)
                sends[ch][some] = packed
        with jax.named_scope("send"):
            dispatch(ch)

    stores = []
    for ch in range(n_chunk):
        with jax.named_scope("wait"):
            arrived(ch)
        with jax.named_scope("final"):
            if ch == 0:
                index_done()
                pick0 = jnp.where(iota((8, 128), 1) == 0, 1.0, 0.0).astype(BF16)
                named = mm_nt(pick0, col_recv[...].astype(F32).reshape(slots, 128).astype(BF16))[:1]
                gather = jnp.where(iota((owned, slots), 0).astype(F32) == named, 1.0, 0.0).astype(BF16)
            got = recvs[ch][...].astype(F32)
            got = jnp.concatenate(
                [got[:, :SLOTS].reshape(slots, 128), got[:, SLOTS:].reshape(slots, 128)], axis=1
            )
            cols = pl.ds(ch * CHUNK, CHUNK)
            result[:, cols] = mm(gather, got.astype(BF16))
        store = pltpu.make_async_copy(result.at[:, cols], out_ref.at[:, cols], load_sem.at[ch])
        store.start()
        stores.append(store)
    for ch in range(n_chunk):
        left_device(ch)
        stores[ch].wait()


def local(coupling_panel, interior_factor, border_rows, target_rows, border_block):
    panel, factor, rows = coupling_panel[0], interior_factor[0], border_rows[0]
    n, width = panel.shape
    holders = lax.axis_size("row") * lax.axis_size("col")
    n_col = lax.axis_size("col")
    n_tile, n_big, n_chunk = n // TILE, n // BIG, width // CHUNK
    pairs = n_big * (n_big - 1) // 2
    hbm = pl.BlockSpec(memory_space=pl.ANY)
    assembled = pl.pallas_call(
        kernel,
        out_shape=jax.ShapeDtypeStruct(border_block.shape, F32),
        in_specs=[hbm] * 4,
        out_specs=hbm,
        scratch_shapes=[
            pltpu.VMEM(panel.shape, BF16),
            pltpu.VMEM(rows.shape, BF16),
            pltpu.VMEM((n_tile, 3, 128, 128), F32),
            pltpu.VMEM((n_big, TILE, TILE), F32),
            pltpu.VMEM((pairs, BIG, BIG), F32),
            pltpu.VMEM((n_big, 3, TILE, TILE), BF16),
            pltpu.VMEM((n_big, 3, TILE, TILE), BF16),
            pltpu.VMEM((pairs, BIG, BIG), BF16),
            pltpu.VMEM((pairs, BIG, BIG), BF16),
            pltpu.VMEM((CHUNK, n), F32),
            pltpu.VMEM((holders * SLOTS, target_rows.shape[1]), BF16),
            pltpu.VMEM((holders, 2 * SLOTS, 128), BF16),
            pltpu.VMEM((holders, 2 * SLOTS, 128), BF16),
            pltpu.VMEM((holders, 2 * SLOTS, 128), BF16),
            pltpu.VMEM((holders, 2 * SLOTS, 128), BF16),
            pltpu.VMEM((n_col, holders // n_col, SLOTS, 128), BF16),
            pltpu.VMEM((n_col, holders // n_col, SLOTS, 128), BF16),
            pltpu.VMEM((holders // n_col, n_col, SLOTS, 128), BF16),
            pltpu.VMEM(target_rows.shape, I32),
            pltpu.VMEM(border_block.shape, F32),
            pltpu.SemaphoreType.DMA((3 * n_tile + n_big + pairs + 3,)),
            pltpu.SemaphoreType.DMA((n_chunk + 2,)),
            pltpu.SemaphoreType.DMA((n_chunk + 2,)),
        ],
        compiler_params=pltpu.CompilerParams(
            collective_id=0, has_side_effects=True, vmem_limit_bytes=53 * 1024 * 1024
        ),
        name="schur_panel",
    )(panel, factor, rows, target_rows)
    return border_block - assembled


def solution(mesh):
    placed = (
        P("row", None, None),
        P("row", None, None),
        P("row", "col", None),
        P("row", "col"),
        P(("row", "col"), None),
    )
    return jax.shard_map(
        local, mesh=mesh, in_specs=placed, out_specs=P(("row", "col"), None), check_vma=False
    )
```

```python
import jax
import jax.numpy as jnp
from jax import lax
from jax.experimental import pallas as pl
from jax.experimental.pallas import tpu as pltpu
from jax.sharding import PartitionSpec as P

F32, BF16, I32 = jnp.float32, jnp.bfloat16, jnp.int32
BASE = 16
TILE = 256
BIG = 512
CHUNK = 256
SLOTS = 8
GROUPS = 2
SIDE = 4
CORES = 2
LOGICAL = pl.DeviceIdType.LOGICAL
EMPTY = -512.0


def iota(shape, axis):
    return lax.broadcasted_iota(I32, shape, axis)


def split(x):
    hi = x.astype(BF16)
    return hi, (x - hi.astype(F32)).astype(BF16)


def mm(a, b):
    return jnp.dot(a, b, preferred_element_type=F32)


def mm_nt(a, b):
    return lax.dot_general(a, b, (((1,), (1,)), ((), ())), preferred_element_type=F32)


def mm3(a, b):
    return mm(a[0], b[0]) + (mm(a[0], b[1]) + mm(a[1], b[0]))


def invert_base(strip):
    rows, width = strip.shape
    lane = iota((rows, width), 1)
    row = iota((rows, width), 0)
    within = lane % BASE
    start = lane - within
    tiles = range(0, width, 128)
    local = (lane - within)[:, :128] % 128

    def pick(x, index):
        return jnp.concatenate(
            [jnp.take_along_axis(x[:, t : t + 128], index[: x.shape[0]], axis=1) for t in tiles], axis=1
        )

    recip = 1.0 / pick(strip, local + row[:, :128])
    scaled = jnp.where(within < row, strip * recip, 0.0)
    inverse = jnp.where(within == row, recip, 0.0)
    for k in range(rows - 1):
        first = (k + 1) // 8 * 8
        factor = pick(scaled[first:], local + k)
        update = inverse[first:] - factor * inverse[k : k + 1]
        inverse = update if first == 0 else jnp.concatenate([inverse[:first], update], axis=0)
    return inverse


def stacked(a, b):
    rows = a[0].shape[0]
    both = mm(jnp.concatenate(a, axis=0), b[0])
    return both[:rows] + (both[rows:] + mm(a[0], b[1]))


def spread(strip, size):
    width = strip[0].shape[1]
    if size == width:
        return strip
    group = iota((size, width), 1) // size
    return tuple(
        jnp.concatenate(
            [part * jnp.where(group == q, 1.0, 0.0).astype(BF16) for q in range(width // size)], axis=0
        )
        for part in strip
    )


def below(corner, first, second, size):
    inner = stacked(split(corner), spread(split(first), size))
    return stacked(split(second), spread(split(inner), size))


def small_tiles(diag):
    return [diag[t, h] for t in range(diag.shape[0]) for h in range(2)]


def invert_bases(diag):
    small = small_tiles(diag)
    group = iota((BASE, 128), 1) // BASE
    strips = []
    for tile in small:
        strip = tile[:BASE]
        for q in range(1, 128 // BASE):
            strip = jnp.where(group == q, tile[q * BASE : (q + 1) * BASE], strip)
        strips.append(strip)
    base = invert_base(jnp.concatenate(strips, axis=1))
    return [base[:, t : t + 128] for t in range(0, base.shape[1], 128)]


def invert_small(diag, tiles, between):
    small = small_tiles(diag)
    size = BASE
    while size < 128:
        between()
        group = iota((size, 128), 1) // size
        even = group % 2 == 0
        corners = []
        for tile in small:
            corner = tile[size : 2 * size]
            for q in range(1, 128 // (2 * size)):
                at = (2 * q + 1) * size
                corner = jnp.where(group == 2 * q, tile[at : at + size], corner)
            corners.append(corner)

        def evens(x):
            return [jnp.where(even, x[t], pltpu.roll(x[t + 1], size, 1)) for t in range(0, len(x), 2)]

        def odds(x):
            return [jnp.where(even, pltpu.roll(x[t], 128 - size, 1), x[t + 1]) for t in range(0, len(x), 2)]

        left = [below(c, f, g, size) for c, f, g in zip(evens(corners), evens(tiles), odds(tiles))]
        merged = []
        for t, tile in enumerate(tiles):
            x = left[t // 2] if t % 2 == 0 else pltpu.roll(left[t // 2], 128 - size, 1)
            merged.append(
                jnp.concatenate([jnp.where(even, tile, 0.0), jnp.where(even, -x, tile)], axis=0)
            )
        tiles = merged
        size *= 2
    return tiles


def invert_tiles(diag, tiles):
    n_tile = diag.shape[0]
    left = [below(diag[t, 2], tiles[2 * t], tiles[2 * t + 1], 128) for t in range(n_tile)]
    zero = jnp.zeros((128, 128), F32)
    return [
        jnp.concatenate(
            [
                jnp.concatenate([tiles[2 * t], zero], axis=1),
                jnp.concatenate([-left[t], tiles[2 * t + 1]], axis=1),
            ],
            axis=0,
        )
        for t in range(n_tile)
    ]


def parts_of(device):
    col = SIDE * SIDE
    return (
        lax.div(device, CORES * col),
        lax.rem(lax.div(device, col), CORES),
        lax.rem(lax.div(device, SIDE), SIDE),
        lax.rem(device, SIDE),
    )


def joined(y, core, x, z):
    return ((y * CORES + core) * SIDE + x) * SIDE + z


SIZES = (SIDE, CORES, SIDE, SIDE)


def steps_of(offset):
    return (
        offset // (CORES * SIDE * SIDE),
        offset // (SIDE * SIDE) % CORES,
        offset // SIDE % SIDE,
        offset % SIDE,
    )


def opposite(offset):
    return joined(*((n - d) % n for n, d in zip(SIZES, steps_of(offset))))


def hops(offset):
    y, core, x, z = steps_of(offset)
    return sum(min(d, SIDE - d) for d in (y, x, z)) + 0.5 * core


def send_order(n):
    classes = {}
    for o in sorted(range(1, n), key=lambda o: -hops(o)):
        y, core, x, z = steps_of(o)
        moved = ("x", x) if x else ("y", y) if y else ("z", z)
        classes.setdefault(moved, []).append(o)
    placed = [((i + 0.5) / len(c), -len(c), o) for c in classes.values() for i, o in enumerate(c)]
    return [o for _, _, o in sorted(placed)]


def kernel(
    panel_hbm, factor_hbm, rows_hbm, target_hbm, out_ref,
    panel, rows, diag, sub, off, vh, vl, oh, ol, fwd, place, send0, recv0, send1, recv1, target_ref, result,
    load_sem, send_sem, recv_sem,
):
    n_holders = lax.axis_size("row") * lax.axis_size("col")
    me = lax.axis_index("row") * lax.axis_size("col") + lax.axis_index("col")
    here = parts_of(me)
    n_big = off.shape[0]
    n_tile = diag.shape[0]
    owned = result.shape[0]
    sends, recvs = (send0, send1), (recv0, recv1)
    pairs = [(1, 0), (2, 0), (2, 1)]
    offsets = send_order(n_holders)
    ahead = [[lax.rem(c + d, n) for d in range(n)] for c, n in zip(here, SIZES)]
    rows_ahead = [joined(y, core, 0, 0) for y in ahead[0] for core in ahead[1]]
    cols_ahead = [joined(0, 0, x, z) for x in ahead[2] for z in ahead[3]]

    def device_at(o):
        return rows_ahead[o // (SIDE * SIDE)] + cols_ahead[o % (SIDE * SIDE)]

    loads = []

    def load(src, dst):
        cp = pltpu.make_async_copy(src, dst, load_sem.at[len(loads)])
        cp.start()
        loads.append(cp)

    def factor_at(r, c, size):
        return factor_hbm.at[pl.ds(r * size, size), pl.ds(c * size, size)]

    load(target_hbm, target_ref)
    for t in range(n_tile):
        load(factor_at(2 * t, 2 * t, 128), diag.at[t, 0])
        load(factor_at(2 * t + 1, 2 * t + 1, 128), diag.at[t, 1])
    for t in range(n_tile):
        load(factor_at(2 * t + 1, 2 * t, 128), diag.at[t, 2])
    for t in range(n_big):
        load(factor_at(2 * t + 1, 2 * t, TILE), sub.at[t])
    for p, (i, j) in enumerate(pairs):
        load(factor_at(i, j, BIG), off.at[p])
    load(panel_hbm, panel)
    load(rows_hbm, rows)

    barrier = pltpu.get_barrier_semaphore()

    @pl.when(me != 0)
    def _():
        pl.semaphore_signal(barrier, inc=1, device_id=0, device_id_type=LOGICAL)

    def collect():
        @pl.when(me == 0)
        def _():
            pl.semaphore_wait(barrier, n_holders - 1)
            for o in range(n_holders - 1, 0, -1):
                pl.semaphore_signal(barrier, inc=1, device_id=o, device_id_type=LOGICAL)

    def all_entered():
        @pl.when(me != 0)
        def _():
            pl.semaphore_wait(barrier, 1)

    first, second = 2 * n_tile + 1, 3 * n_tile + n_big + 1
    loads[0].wait()
    with jax.named_scope("place"):
        sent = target_ref.shape[1]
        target = jnp.broadcast_to(target_ref[...], (8, sent))
        holder = target // owned
        within = target - holder * owned
        lane = iota((8, sent), 1)
        rank = jnp.zeros((8, sent), I32)
        for d in range(1, SLOTS):
            same = (pltpu.roll(holder, d, 1) == holder) & (lane >= d)
            rank = rank + jnp.where(same, 1, 0)
        away = joined(*(lax.rem(h - c + n, n) for h, c, n in zip(parts_of(holder), here, SIZES)))
        position = (away * SLOTS + rank)[:1]
        slots = n_holders * SLOTS
        placed = jnp.where(iota((slots, sent), 0) == position, 1.0, 0.0).astype(BF16)
        place[...] = placed
        described = jnp.concatenate(
            [jnp.broadcast_to(within[:1].astype(F32), (128, sent)), jnp.ones((128, sent), F32)], axis=0
        ).astype(BF16)
        found = mm_nt(placed, described)
        index = found[:, :128] + EMPTY * (1.0 - found[:, 128:])
        send0[:, 2 * SLOTS :] = index.reshape(n_holders, SLOTS, 128).astype(BF16)
    for cp in loads[1:first]:
        cp.wait()
    waiting = loads[first:second]

    def between():
        waiting.pop(0).wait()

    with jax.named_scope("small"):
        small = invert_small(diag, invert_bases(diag), between)
    for cp in waiting:
        cp.wait()
    with jax.named_scope("merge"):
        inverse = invert_tiles(diag, small)
        for b in range(n_big):
            left = split(below(sub[b], inverse[2 * b], inverse[2 * b + 1], TILE))
            top, bottom = split(inverse[2 * b]), split(inverse[2 * b + 1])
            for ref, i in ((vh, 0), (vl, 1)):
                ref[b, 0] = top[i]
                ref[b, 1] = left[i]
                ref[b, 2] = bottom[i]
    for cp in loads[second:]:
        cp.wait()
    with jax.named_scope("collect"):
        collect()
    with jax.named_scope("split"):
        for p in range(len(pairs)):
            oh[p], ol[p] = split(off[p])
    def dispatch(ch):
        for o in offsets:
            pltpu.make_async_remote_copy(
                src_ref=sends[ch].at[o],
                dst_ref=recvs[ch].at[opposite(o)],
                send_sem=send_sem.at[ch],
                recv_sem=recv_sem.at[ch],
                device_id=device_at(o),
                device_id_type=LOGICAL,
            ).start()
        recvs[ch][0] = sends[ch][0]

    others = pl.ds(1, n_holders - 1)

    def arrived(ch):
        pltpu.make_async_copy(sends[ch].at[others], recvs[ch].at[others], recv_sem.at[ch]).wait()

    def left_device(ch):
        pltpu.make_async_copy(sends[ch].at[others], recvs[ch].at[others], send_sem.at[ch]).wait()

    def inv(b, part):
        return (vh[b, part], vl[b, part])

    def halves(x, axis):
        if axis == 0:
            return [tuple(y[:TILE] for y in x), tuple(y[TILE:] for y in x)]
        return [tuple(y[:, :TILE] for y in x), tuple(y[:, TILE:] for y in x)]

    n_chunk = len(sends)
    for ch in range(n_chunk):
        with jax.named_scope("fwd"):
            cols = slice(ch * CHUNK, (ch + 1) * CHUNK)
            rhs = [panel[b * BIG : (b + 1) * BIG, cols].astype(F32) for b in range(n_big)]
            for b in range(n_big):
                r = halves(split(rhs[b]), 0)
                upper = mm3(inv(b, 0), r[0])
                lower = mm3(inv(b, 2), r[1]) - mm3(inv(b, 1), r[0])
                f = jnp.concatenate([upper, lower], axis=0)
                fwd[:, b * BIG : (b + 1) * BIG] = f.T
                fs = halves(split(f), 0)
                for p, (i, j) in enumerate(pairs):
                    if j == b:
                        o = halves((oh[p], ol[p]), 1)
                        rhs[i] = (rhs[i] - mm3(o[0], fs[0])) - mm3(o[1], fs[1])
        with jax.named_scope("bwd"):
            partial = []
            for b in reversed(range(n_big)):
                q = halves(split(fwd[:, b * BIG : (b + 1) * BIG]), 1)
                first = mm3(q[0], inv(b, 0)) - mm3(q[1], inv(b, 1))
                second = mm3(q[1], inv(b, 2))
                x = jnp.concatenate([first, second], axis=1)
                xs = halves(split(x), 1)
                for p, (i, j) in reversed(list(enumerate(pairs))):
                    if i == b:
                        at = slice(j * BIG, (j + 1) * BIG)
                        o = halves((oh[p], ol[p]), 0)
                        fwd[:, at] = (fwd[:, at] - mm3(xs[0], o[0])) - mm3(xs[1], o[1])
                at = b * BIG
                if b:
                    partial.append(mm_nt(rows[:, at : at + BIG], jnp.concatenate([-xs[0][0], -xs[1][0]], axis=1)))
                else:
                    update = mm_nt(rows[:, :TILE], xs[0][0]) - mm_nt(rows[:, TILE:BIG], -xs[1][0])
            for other in partial:
                update = update - other
            update = update.astype(BF16)
        with jax.named_scope("pack"):
            step = n_holders // GROUPS
            for g in range(GROUPS):
                some = slice(g * step, (g + 1) * step)
                packed = mm(place[g * step * SLOTS : (g + 1) * step * SLOTS], update).reshape(step, SLOTS, CHUNK)
                packed = jnp.concatenate([packed[:, :, :128], packed[:, :, 128:]], axis=1).astype(BF16)
                sends[ch][some, : 2 * SLOTS] = packed
        with jax.named_scope("send"):
            if ch == 0:
                all_entered()
            dispatch(ch)

    stores = []
    for ch in range(n_chunk):
        with jax.named_scope("wait"):
            arrived(ch)
        with jax.named_scope("final"):
            if ch == 0:
                pick0 = jnp.where(iota((8, 128), 1) == 0, 1.0, 0.0).astype(BF16)
                named = mm_nt(pick0, recv0[:, 2 * SLOTS :].astype(F32).reshape(slots, 128).astype(BF16))[:1]
                gather = jnp.where(iota((owned, slots), 0).astype(F32) == named, 1.0, 0.0).astype(BF16)
            got = recvs[ch][:, : 2 * SLOTS].astype(F32)
            got = jnp.concatenate(
                [got[:, :SLOTS].reshape(slots, 128), got[:, SLOTS:].reshape(slots, 128)], axis=1
            )
            cols = pl.ds(ch * CHUNK, CHUNK)
            result[:, cols] = mm(gather, got.astype(BF16))
        store = pltpu.make_async_copy(result.at[:, cols], out_ref.at[:, cols], load_sem.at[ch])
        store.start()
        stores.append(store)
    for ch in range(n_chunk):
        left_device(ch)
        stores[ch].wait()


def local(coupling_panel, interior_factor, border_rows, target_rows, border_block):
    panel, factor, rows = coupling_panel[0], interior_factor[0], border_rows[0]
    n, width = panel.shape
    holders = lax.axis_size("row") * lax.axis_size("col")
    n_tile, n_big, n_chunk = n // TILE, n // BIG, width // CHUNK
    pairs = n_big * (n_big - 1) // 2
    hbm = pl.BlockSpec(memory_space=pl.ANY)
    assembled = pl.pallas_call(
        kernel,
        out_shape=jax.ShapeDtypeStruct(border_block.shape, F32),
        in_specs=[hbm] * 4,
        out_specs=hbm,
        scratch_shapes=[
            pltpu.VMEM(panel.shape, BF16),
            pltpu.VMEM(rows.shape, BF16),
            pltpu.VMEM((n_tile, 3, 128, 128), F32),
            pltpu.VMEM((n_big, TILE, TILE), F32),
            pltpu.VMEM((pairs, BIG, BIG), F32),
            pltpu.VMEM((n_big, 3, TILE, TILE), BF16),
            pltpu.VMEM((n_big, 3, TILE, TILE), BF16),
            pltpu.VMEM((pairs, BIG, BIG), BF16),
            pltpu.VMEM((pairs, BIG, BIG), BF16),
            pltpu.VMEM((CHUNK, n), F32),
            pltpu.VMEM((holders * SLOTS, target_rows.shape[1]), BF16),
            pltpu.VMEM((holders, 3 * SLOTS, 128), BF16),
            pltpu.VMEM((holders, 3 * SLOTS, 128), BF16),
            pltpu.VMEM((holders, 2 * SLOTS, 128), BF16),
            pltpu.VMEM((holders, 2 * SLOTS, 128), BF16),
            pltpu.VMEM(target_rows.shape, I32),
            pltpu.VMEM(border_block.shape, F32),
            pltpu.SemaphoreType.DMA((3 * n_tile + n_big + pairs + 3,)),
            pltpu.SemaphoreType.DMA((n_chunk,)),
            pltpu.SemaphoreType.DMA((n_chunk,)),
        ],
        compiler_params=pltpu.CompilerParams(
            collective_id=0, has_side_effects=True, vmem_limit_bytes=53 * 1024 * 1024
        ),
        name="schur_panel",
    )(panel, factor, rows, target_rows)
    return border_block - assembled


def solution(mesh):
    placed = (
        P("row", None, None),
        P("row", None, None),
        P("row", "col", None),
        P("row", "col"),
        P(("row", "col"), None),
    )
    return jax.shard_map(
        local, mesh=mesh, in_specs=placed, out_specs=P(("row", "col"), None), check_vma=False
    )
```

```python
import jax
import jax.numpy as jnp
from jax import lax
from jax.experimental import pallas as pl
from jax.experimental.pallas import tpu as pltpu
from jax.sharding import PartitionSpec as P

F32, BF16, I32 = jnp.float32, jnp.bfloat16, jnp.int32
BASE = 16
TILE = 256
BIG = 512
CHUNK = 256
SLOTS = 8
GROUPS = 2
SIDE = 4
CORES = 2
LOGICAL = pl.DeviceIdType.LOGICAL
EMPTY = -512.0


def iota(shape, axis):
    return lax.broadcasted_iota(I32, shape, axis)


def split(x):
    hi = x.astype(BF16)
    return hi, (x - hi.astype(F32)).astype(BF16)


def mm(a, b):
    return jnp.dot(a, b, preferred_element_type=F32)


def mm_nt(a, b):
    return lax.dot_general(a, b, (((1,), (1,)), ((), ())), preferred_element_type=F32)


def mm3(a, b):
    return mm(a[0], b[0]) + (mm(a[0], b[1]) + mm(a[1], b[0]))


def invert_base(strip):
    rows, width = strip.shape
    lane = iota((rows, width), 1)
    row = iota((rows, width), 0)
    within = lane % BASE
    start = lane - within
    tiles = range(0, width, 128)
    local = (lane - within)[:, :128] % 128

    def pick(x, index):
        return jnp.concatenate(
            [jnp.take_along_axis(x[:, t : t + 128], index[: x.shape[0]], axis=1) for t in tiles], axis=1
        )

    recip = 1.0 / pick(strip, local + row[:, :128])
    scaled = jnp.where(within < row, strip * recip, 0.0)
    inverse = jnp.where(within == row, recip, 0.0)
    for k in range(rows - 1):
        first = (k + 1) // 8 * 8
        factor = pick(scaled[first:], local + k)
        update = inverse[first:] - factor * inverse[k : k + 1]
        inverse = update if first == 0 else jnp.concatenate([inverse[:first], update], axis=0)
    return inverse


def stacked(a, b):
    rows = a[0].shape[0]
    both = mm(jnp.concatenate(a, axis=0), b[0])
    return both[:rows] + (both[rows:] + mm(a[0], b[1]))


def spread(strip, size):
    width = strip[0].shape[1]
    if size == width:
        return strip
    group = iota((size, width), 1) // size
    return tuple(
        jnp.concatenate(
            [part * jnp.where(group == q, 1.0, 0.0).astype(BF16) for q in range(width // size)], axis=0
        )
        for part in strip
    )


def below(corner, first, second, size):
    inner = stacked(split(corner), spread(split(first), size))
    return stacked(split(second), spread(split(inner), size))


def small_tiles(diag):
    return [diag[t, h] for t in range(diag.shape[0]) for h in range(2)]


def invert_bases(diag):
    small = small_tiles(diag)
    group = iota((BASE, 128), 1) // BASE
    strips = []
    for tile in small:
        strip = tile[:BASE]
        for q in range(1, 128 // BASE):
            strip = jnp.where(group == q, tile[q * BASE : (q + 1) * BASE], strip)
        strips.append(strip)
    base = invert_base(jnp.concatenate(strips, axis=1))
    return [base[:, t : t + 128] for t in range(0, base.shape[1], 128)]


def invert_small(diag, tiles):
    small = small_tiles(diag)
    size = BASE
    while size < 128:
        group = iota((size, 128), 1) // size
        even = group % 2 == 0
        corners = []
        for tile in small:
            corner = tile[size : 2 * size]
            for q in range(1, 128 // (2 * size)):
                at = (2 * q + 1) * size
                corner = jnp.where(group == 2 * q, tile[at : at + size], corner)
            corners.append(corner)

        def evens(x):
            return [jnp.where(even, x[t], pltpu.roll(x[t + 1], size, 1)) for t in range(0, len(x), 2)]

        def odds(x):
            return [jnp.where(even, pltpu.roll(x[t], 128 - size, 1), x[t + 1]) for t in range(0, len(x), 2)]

        left = [below(c, f, g, size) for c, f, g in zip(evens(corners), evens(tiles), odds(tiles))]
        merged = []
        for t, tile in enumerate(tiles):
            x = left[t // 2] if t % 2 == 0 else pltpu.roll(left[t // 2], 128 - size, 1)
            merged.append(
                jnp.concatenate([jnp.where(even, tile, 0.0), jnp.where(even, -x, tile)], axis=0)
            )
        tiles = merged
        size *= 2
    return tiles


def invert_tiles(diag, tiles):
    n_tile = diag.shape[0]
    left = [below(diag[t, 2], tiles[2 * t], tiles[2 * t + 1], 128) for t in range(n_tile)]
    zero = jnp.zeros((128, 128), F32)
    return [
        jnp.concatenate(
            [
                jnp.concatenate([tiles[2 * t], zero], axis=1),
                jnp.concatenate([-left[t], tiles[2 * t + 1]], axis=1),
            ],
            axis=0,
        )
        for t in range(n_tile)
    ]


def parts_of(device):
    col = SIDE * SIDE
    return (
        lax.div(device, CORES * col),
        lax.rem(lax.div(device, col), CORES),
        lax.rem(lax.div(device, SIDE), SIDE),
        lax.rem(device, SIDE),
    )


def joined(y, core, x, z):
    return ((y * CORES + core) * SIDE + x) * SIDE + z


SIZES = (SIDE, CORES, SIDE, SIDE)


def steps_of(offset):
    return (
        offset // (CORES * SIDE * SIDE),
        offset // (SIDE * SIDE) % CORES,
        offset // SIDE % SIDE,
        offset % SIDE,
    )


def opposite(offset):
    return joined(*((n - d) % n for n, d in zip(SIZES, steps_of(offset))))


def hops(offset):
    y, core, x, z = steps_of(offset)
    return sum(min(d, SIDE - d) for d in (y, x, z)) + 0.5 * core


def send_order(n):
    classes = {}
    for o in sorted(range(1, n), key=lambda o: -hops(o)):
        y, core, x, z = steps_of(o)
        moved = ("x", x) if x else ("y", y) if y else ("z", z)
        classes.setdefault(moved, []).append(o)
    placed = [((i + 0.5) / len(c), -len(c), o) for c in classes.values() for i, o in enumerate(c)]
    return [o for _, _, o in sorted(placed)]


def kernel(
    panel_hbm, factor_hbm, rows_hbm, target_hbm, out_ref,
    panel, rows, diag, sub, off, vh, vl, oh, ol, fwd, place, send0, recv0, send1, recv1,
    row_send, row_recv, col_send, col_recv, target_ref, result,
    load_sem, send_sem, recv_sem,
):
    n_holders = lax.axis_size("row") * lax.axis_size("col")
    me = lax.axis_index("row") * lax.axis_size("col") + lax.axis_index("col")
    here = parts_of(me)
    n_col = SIDE * SIDE
    n_row = n_holders // n_col
    n_big = off.shape[0]
    n_tile = diag.shape[0]
    owned = result.shape[0]
    sends, recvs = (send0, send1), (recv0, recv1)
    n_chunk = len(sends)
    pairs = [(1, 0), (2, 0), (2, 1)]
    offsets = send_order(n_holders)
    ahead = [[lax.rem(c + d, n) for d in range(n)] for c, n in zip(here, SIZES)]
    rows_ahead = [joined(y, core, 0, 0) for y in ahead[0] for core in ahead[1]]
    cols_ahead = [joined(0, 0, x, z) for x in ahead[2] for z in ahead[3]]

    def device_at(o):
        return rows_ahead[o // (SIDE * SIDE)] + cols_ahead[o % (SIDE * SIDE)]

    loads = []

    def load(src, dst):
        cp = pltpu.make_async_copy(src, dst, load_sem.at[len(loads)])
        cp.start()
        loads.append(cp)

    def factor_at(r, c, size):
        return factor_hbm.at[pl.ds(r * size, size), pl.ds(c * size, size)]

    load(target_hbm, target_ref)
    for t in range(n_tile):
        load(factor_at(2 * t, 2 * t, 128), diag.at[t, 0])
        load(factor_at(2 * t + 1, 2 * t + 1, 128), diag.at[t, 1])
    for t in range(n_tile):
        load(factor_at(2 * t + 1, 2 * t, 128), diag.at[t, 2])
    for t in range(n_big):
        load(factor_at(2 * t + 1, 2 * t, TILE), sub.at[t])
    for p, (i, j) in enumerate(pairs):
        load(factor_at(i, j, BIG), off.at[p])
    load(panel_hbm, panel)
    load(rows_hbm, rows)

    with jax.named_scope("greet"):
        barrier = pltpu.get_barrier_semaphore()
        for o in offsets:
            pl.semaphore_signal(barrier, inc=1, device_id=device_at(o), device_id_type=LOGICAL)

    first, second = 2 * n_tile + 1, 3 * n_tile + n_big + 1
    for cp in loads[:first]:
        cp.wait()
    with jax.named_scope("place"):
        sent = target_ref.shape[1]
        target = jnp.broadcast_to(target_ref[...], (8, sent))
        holder = target // owned
        within = target - holder * owned
        lane = iota((8, sent), 1)
        rank = jnp.zeros((8, sent), I32)
        for d in range(1, SLOTS):
            same = (pltpu.roll(holder, d, 1) == holder) & (lane >= d)
            rank = rank + jnp.where(same, 1, 0)
        away = joined(*(lax.rem(h - c + n, n) for h, c, n in zip(parts_of(holder), here, SIZES)))
        position = (away * SLOTS + rank)[:1]
        slots = n_holders * SLOTS
        placed = jnp.where(iota((slots, sent), 0) == position, 1.0, 0.0).astype(BF16)
        place[...] = placed
        described = jnp.concatenate(
            [jnp.broadcast_to(within[:1].astype(F32), (128, sent)), jnp.ones((128, sent), F32)], axis=0
        ).astype(BF16)
        found = mm_nt(placed, described)
        index = found[:, :128] + EMPTY * (1.0 - found[:, 128:])
        index = jnp.where(iota((slots, 128), 1) == iota((slots, 128), 0) % SLOTS, index, 0.0).astype(BF16)
        turn = iota((n_holders, slots), 0)
        turn = turn % n_row * n_col + turn // n_row
        collect = jnp.where(turn == iota((n_holders, slots), 1) // SLOTS, 1.0, 0.0).astype(BF16)
        row_send[...] = mm(collect, index).reshape(n_col, n_row, 128)
    with jax.named_scope("small"):
        small = invert_small(diag, invert_bases(diag))
    for cp in loads[first:second]:
        cp.wait()
    with jax.named_scope("merge"):
        inverse = invert_tiles(diag, small)
        for b in range(n_big):
            left = split(below(sub[b], inverse[2 * b], inverse[2 * b + 1], TILE))
            top, bottom = split(inverse[2 * b]), split(inverse[2 * b + 1])
            for ref, i in ((vh, 0), (vl, 1)):
                ref[b, 0] = top[i]
                ref[b, 1] = left[i]
                ref[b, 2] = bottom[i]
    for cp in loads[second:]:
        cp.wait()
    with jax.named_scope("split"):
        for p in range(len(pairs)):
            oh[p], ol[p] = split(off[p])
    def dispatch(ch):
        for o in offsets:
            pltpu.make_async_remote_copy(
                src_ref=sends[ch].at[o],
                dst_ref=recvs[ch].at[opposite(o)],
                send_sem=send_sem.at[ch],
                recv_sem=recv_sem.at[ch],
                device_id=device_at(o),
                device_id_type=LOGICAL,
            ).start()
        recvs[ch][0] = sends[ch][0]

    others = pl.ds(1, n_holders - 1)

    def arrived(ch):
        pltpu.make_async_copy(sends[ch].at[others], recvs[ch].at[others], recv_sem.at[ch]).wait()

    def left_device(ch):
        pltpu.make_async_copy(sends[ch].at[others], recvs[ch].at[others], send_sem.at[ch]).wait()

    def start(src, dst, o, at):
        pltpu.make_async_remote_copy(
            src_ref=src, dst_ref=dst, send_sem=send_sem.at[at], recv_sem=recv_sem.at[at],
            device_id=device_at(o), device_id_type=LOGICAL,
        ).start()

    col_peers, row_peers = pl.ds(1, n_col - 1), pl.ds(1, n_row - 1)

    def index_to_row():
        for o in range(1, n_col):
            start(row_send.at[o], row_recv.at[opposite(o)], o, n_chunk)
        row_recv[0] = row_send[0]

    def index_to_col():
        pltpu.make_async_copy(row_send.at[col_peers], row_recv.at[col_peers], recv_sem.at[n_chunk]).wait()
        turn = iota((n_holders, n_holders), 0)
        turn = turn % n_col * n_row + turn // n_col
        turned = jnp.where(turn == iota((n_holders, n_holders), 1), 1.0, 0.0).astype(BF16)
        col_send[...] = mm(turned, row_recv[...].reshape(n_holders, 128).astype(BF16)).reshape(n_row, n_col, 128)
        for r in range(1, n_row):
            start(col_send.at[r], col_recv.at[opposite(r * n_col) // n_col], r * n_col, n_chunk + 1)
        col_recv[0] = col_send[0]

    def index_done():
        pltpu.make_async_copy(row_send.at[col_peers], row_recv.at[col_peers], send_sem.at[n_chunk]).wait()
        for sem in (recv_sem, send_sem):
            pltpu.make_async_copy(col_send.at[row_peers], col_recv.at[row_peers], sem.at[n_chunk + 1]).wait()

    def inv(b, part):
        return (vh[b, part], vl[b, part])

    def halves(x, axis):
        if axis == 0:
            return [tuple(y[:TILE] for y in x), tuple(y[TILE:] for y in x)]
        return [tuple(y[:, :TILE] for y in x), tuple(y[:, TILE:] for y in x)]

    n_chunk = len(sends)
    for ch in range(n_chunk):
        with jax.named_scope("fwd"):
            cols = slice(ch * CHUNK, (ch + 1) * CHUNK)
            rhs = [panel[b * BIG : (b + 1) * BIG, cols].astype(F32) for b in range(n_big)]
            for b in range(n_big):
                r = halves(split(rhs[b]), 0)
                upper = mm3(inv(b, 0), r[0])
                lower = mm3(inv(b, 2), r[1]) - mm3(inv(b, 1), r[0])
                f = jnp.concatenate([upper, lower], axis=0)
                fwd[:, b * BIG : (b + 1) * BIG] = f.T
                fs = halves(split(f), 0)
                for p, (i, j) in enumerate(pairs):
                    if j == b:
                        o = halves((oh[p], ol[p]), 1)
                        rhs[i] = (rhs[i] - mm3(o[0], fs[0])) - mm3(o[1], fs[1])
        with jax.named_scope("idx"):
            if ch == 0:
                pl.semaphore_wait(barrier, n_holders - 1)
                index_to_row()
            else:
                index_to_col()
        with jax.named_scope("bwd"):
            partial = []
            for b in reversed(range(n_big)):
                q = halves(split(fwd[:, b * BIG : (b + 1) * BIG]), 1)
                first = mm3(q[0], inv(b, 0)) - mm3(q[1], inv(b, 1))
                second = mm3(q[1], inv(b, 2))
                x = jnp.concatenate([first, second], axis=1)
                xs = halves(split(x), 1)
                for p, (i, j) in reversed(list(enumerate(pairs))):
                    if i == b:
                        at = slice(j * BIG, (j + 1) * BIG)
                        o = halves((oh[p], ol[p]), 0)
                        fwd[:, at] = (fwd[:, at] - mm3(xs[0], o[0])) - mm3(xs[1], o[1])
                at = b * BIG
                if b:
                    partial.append(mm_nt(rows[:, at : at + BIG], jnp.concatenate([-xs[0][0], -xs[1][0]], axis=1)))
                else:
                    update = mm_nt(rows[:, :TILE], xs[0][0]) - mm_nt(rows[:, TILE:BIG], -xs[1][0])
            for other in partial:
                update = update - other
            update = update.astype(BF16)
        with jax.named_scope("pack"):
            step = n_holders // GROUPS
            for g in range(GROUPS):
                some = slice(g * step, (g + 1) * step)
                packed = mm(place[g * step * SLOTS : (g + 1) * step * SLOTS], update).reshape(step, SLOTS, CHUNK)
                packed = jnp.concatenate([packed[:, :, :128], packed[:, :, 128:]], axis=1).astype(BF16)
                sends[ch][some] = packed
        with jax.named_scope("send"):
            dispatch(ch)

    stores = []
    for ch in range(n_chunk):
        with jax.named_scope("wait"):
            arrived(ch)
        with jax.named_scope("final"):
            if ch == 0:
                index_done()
                names = col_recv[...].reshape(n_holders, 128).astype(BF16)
                lanes = jnp.where(iota((128, slots), 0) == iota((128, slots), 1) % SLOTS, 1.0, 0.0).astype(BF16)
                mine = iota((n_holders, slots), 0) == iota((n_holders, slots), 1) // SLOTS
                named = jnp.sum(jnp.where(mine, mm(names, lanes), 0.0), axis=0, keepdims=True)
                gather = jnp.where(iota((owned, slots), 0).astype(F32) == named, 1.0, 0.0).astype(BF16)
            got = recvs[ch][...].astype(F32)
            got = jnp.concatenate(
                [got[:, :SLOTS].reshape(slots, 128), got[:, SLOTS:].reshape(slots, 128)], axis=1
            )
            cols = pl.ds(ch * CHUNK, CHUNK)
            result[:, cols] = mm(gather, got.astype(BF16))
        store = pltpu.make_async_copy(result.at[:, cols], out_ref.at[:, cols], load_sem.at[ch])
        store.start()
        stores.append(store)
    for ch in range(n_chunk):
        left_device(ch)
        stores[ch].wait()


def local(coupling_panel, interior_factor, border_rows, target_rows, border_block):
    panel, factor, rows = coupling_panel[0], interior_factor[0], border_rows[0]
    n, width = panel.shape
    holders = lax.axis_size("row") * lax.axis_size("col")
    n_col = lax.axis_size("col")
    n_tile, n_big, n_chunk = n // TILE, n // BIG, width // CHUNK
    pairs = n_big * (n_big - 1) // 2
    hbm = pl.BlockSpec(memory_space=pl.ANY)
    assembled = pl.pallas_call(
        kernel,
        out_shape=jax.ShapeDtypeStruct(border_block.shape, F32),
        in_specs=[hbm] * 4,
        out_specs=hbm,
        scratch_shapes=[
            pltpu.VMEM(panel.shape, BF16),
            pltpu.VMEM(rows.shape, BF16),
            pltpu.VMEM((n_tile, 3, 128, 128), F32),
            pltpu.VMEM((n_big, TILE, TILE), F32),
            pltpu.VMEM((pairs, BIG, BIG), F32),
            pltpu.VMEM((n_big, 3, TILE, TILE), BF16),
            pltpu.VMEM((n_big, 3, TILE, TILE), BF16),
            pltpu.VMEM((pairs, BIG, BIG), BF16),
            pltpu.VMEM((pairs, BIG, BIG), BF16),
            pltpu.VMEM((CHUNK, n), F32),
            pltpu.VMEM((holders * SLOTS, target_rows.shape[1]), BF16),
            pltpu.VMEM((holders, 2 * SLOTS, 128), BF16),
            pltpu.VMEM((holders, 2 * SLOTS, 128), BF16),
            pltpu.VMEM((holders, 2 * SLOTS, 128), BF16),
            pltpu.VMEM((holders, 2 * SLOTS, 128), BF16),
            pltpu.VMEM((n_col, holders // n_col, 128), F32),
            pltpu.VMEM((n_col, holders // n_col, 128), F32),
            pltpu.VMEM((holders // n_col, n_col, 128), F32),
            pltpu.VMEM((holders // n_col, n_col, 128), F32),
            pltpu.VMEM(target_rows.shape, I32),
            pltpu.VMEM(border_block.shape, F32),
            pltpu.SemaphoreType.DMA((3 * n_tile + n_big + pairs + 3,)),
            pltpu.SemaphoreType.DMA((n_chunk + 2,)),
            pltpu.SemaphoreType.DMA((n_chunk + 2,)),
        ],
        compiler_params=pltpu.CompilerParams(
            collective_id=0, has_side_effects=True, vmem_limit_bytes=53 * 1024 * 1024
        ),
        name="schur_panel",
    )(panel, factor, rows, target_rows)
    return border_block - assembled


def solution(mesh):
    placed = (
        P("row", None, None),
        P("row", None, None),
        P("row", "col", None),
        P("row", "col"),
        P(("row", "col"), None),
    )
    return jax.shard_map(
        local, mesh=mesh, in_specs=placed, out_specs=P(("row", "col"), None), check_vma=False
    )
```

```python
import jax
import jax.numpy as jnp
from jax import lax
from jax.experimental import pallas as pl
from jax.experimental.pallas import tpu as pltpu
from jax.sharding import PartitionSpec as P

F32, BF16, I32 = jnp.float32, jnp.bfloat16, jnp.int32
BASE = 16
TILE = 256
BIG = 512
CHUNK = 256
PIECES = ((0, 0, 256), (1, 0, 256))
SLOTS = 8
GROUPS = 2
SIDE = 4
CORES = 2
LOGICAL = pl.DeviceIdType.LOGICAL
EMPTY = -512.0


def iota(shape, axis):
    return lax.broadcasted_iota(I32, shape, axis)


def split(x):
    hi = x.astype(BF16)
    return hi, (x - hi.astype(F32)).astype(BF16)


def mm(a, b):
    return jnp.dot(a, b, preferred_element_type=F32)


def mm_nt(a, b):
    return lax.dot_general(a, b, (((1,), (1,)), ((), ())), preferred_element_type=F32)


def mm3(a, b):
    return mm(a[0], b[0]) + (mm(a[0], b[1]) + mm(a[1], b[0]))


def invert_base(strip):
    rows, width = strip.shape
    lane = iota((rows, width), 1)
    row = iota((rows, width), 0)
    within = lane % BASE
    start = lane - within
    tiles = range(0, width, 128)
    local = (lane - within)[:, :128] % 128

    def pick(x, index):
        return jnp.concatenate(
            [jnp.take_along_axis(x[:, t : t + 128], index[: x.shape[0]], axis=1) for t in tiles], axis=1
        )

    recip = 1.0 / pick(strip, local + row[:, :128])
    scaled = jnp.where(within < row, strip * recip, 0.0)
    inverse = jnp.where(within == row, recip, 0.0)
    for k in range(rows - 1):
        first = (k + 1) // 8 * 8
        factor = pick(scaled[first:], local + k)
        update = inverse[first:] - factor * inverse[k : k + 1]
        inverse = update if first == 0 else jnp.concatenate([inverse[:first], update], axis=0)
    return inverse


def stacked(a, b):
    rows = a[0].shape[0]
    both = mm(jnp.concatenate(a, axis=0), b[0])
    return both[:rows] + (both[rows:] + mm(a[0], b[1]))


def spread(strip, size):
    width = strip[0].shape[1]
    if size == width:
        return strip
    group = iota((size, width), 1) // size
    return tuple(
        jnp.concatenate(
            [part * jnp.where(group == q, 1.0, 0.0).astype(BF16) for q in range(width // size)], axis=0
        )
        for part in strip
    )


def below(corner, first, second, size):
    inner = stacked(split(corner), spread(split(first), size))
    return stacked(split(second), spread(split(inner), size))


def small_tiles(diag):
    return [diag[t, h] for t in range(diag.shape[0]) for h in range(2)]


def invert_bases(diag):
    small = small_tiles(diag)
    group = iota((BASE, 128), 1) // BASE
    strips = []
    for tile in small:
        strip = tile[:BASE]
        for q in range(1, 128 // BASE):
            strip = jnp.where(group == q, tile[q * BASE : (q + 1) * BASE], strip)
        strips.append(strip)
    base = invert_base(jnp.concatenate(strips, axis=1))
    return [base[:, t : t + 128] for t in range(0, base.shape[1], 128)]


def invert_small(diag, tiles):
    small = small_tiles(diag)
    size = BASE
    while size < 128:
        group = iota((size, 128), 1) // size
        even = group % 2 == 0
        corners = []
        for tile in small:
            corner = tile[size : 2 * size]
            for q in range(1, 128 // (2 * size)):
                at = (2 * q + 1) * size
                corner = jnp.where(group == 2 * q, tile[at : at + size], corner)
            corners.append(corner)

        def evens(x):
            return [jnp.where(even, x[t], pltpu.roll(x[t + 1], size, 1)) for t in range(0, len(x), 2)]

        def odds(x):
            return [jnp.where(even, pltpu.roll(x[t], 128 - size, 1), x[t + 1]) for t in range(0, len(x), 2)]

        left = [below(c, f, g, size) for c, f, g in zip(evens(corners), evens(tiles), odds(tiles))]
        merged = []
        for t, tile in enumerate(tiles):
            x = left[t // 2] if t % 2 == 0 else pltpu.roll(left[t // 2], 128 - size, 1)
            merged.append(
                jnp.concatenate([jnp.where(even, tile, 0.0), jnp.where(even, -x, tile)], axis=0)
            )
        tiles = merged
        size *= 2
    return tiles


def invert_tiles(diag, tiles):
    n_tile = diag.shape[0]
    left = [below(diag[t, 2], tiles[2 * t], tiles[2 * t + 1], 128) for t in range(n_tile)]
    zero = jnp.zeros((128, 128), F32)
    return [
        jnp.concatenate(
            [
                jnp.concatenate([tiles[2 * t], zero], axis=1),
                jnp.concatenate([-left[t], tiles[2 * t + 1]], axis=1),
            ],
            axis=0,
        )
        for t in range(n_tile)
    ]


def parts_of(device):
    col = SIDE * SIDE
    return (
        lax.div(device, CORES * col),
        lax.rem(lax.div(device, col), CORES),
        lax.rem(lax.div(device, SIDE), SIDE),
        lax.rem(device, SIDE),
    )


def joined(y, core, x, z):
    return ((y * CORES + core) * SIDE + x) * SIDE + z


SIZES = (SIDE, CORES, SIDE, SIDE)


def steps_of(offset):
    return (
        offset // (CORES * SIDE * SIDE),
        offset // (SIDE * SIDE) % CORES,
        offset // SIDE % SIDE,
        offset % SIDE,
    )


def opposite(offset):
    return joined(*((n - d) % n for n, d in zip(SIZES, steps_of(offset))))


def hops(offset):
    y, core, x, z = steps_of(offset)
    return sum(min(d, SIDE - d) for d in (y, x, z)) + 0.5 * core


def send_order(n):
    classes = {}
    for o in sorted(range(1, n), key=lambda o: -hops(o)):
        y, core, x, z = steps_of(o)
        moved = ("x", x) if x else ("y", y) if y else ("z", z)
        classes.setdefault(moved, []).append(o)
    placed = [((i + 0.5) / len(c), -len(c), o) for c in classes.values() for i, o in enumerate(c)]
    return [o for _, _, o in sorted(placed)]


def kernel(
    panel_hbm, factor_hbm, rows_hbm, target_hbm, out_ref,
    panel, rows, diag, sub, off, vh, vl, oh, ol, fwd, place, send0, recv0, send1, recv1,
    row_send, row_recv, col_send, col_recv, target_ref, result,
    load_sem, send_sem, recv_sem,
):
    n_holders = lax.axis_size("row") * lax.axis_size("col")
    me = lax.axis_index("row") * lax.axis_size("col") + lax.axis_index("col")
    here = parts_of(me)
    n_col = SIDE * SIDE
    n_row = n_holders // n_col
    n_big = off.shape[0]
    n_tile = diag.shape[0]
    owned = result.shape[0]
    sends, recvs = (send0, send1), (recv0, recv1)
    n_chunk = len(sends)
    pairs = [(1, 0), (2, 0), (2, 1)]
    offsets = send_order(n_holders)
    ahead = [[lax.rem(c + d, n) for d in range(n)] for c, n in zip(here, SIZES)]
    rows_ahead = [joined(y, core, 0, 0) for y in ahead[0] for core in ahead[1]]
    cols_ahead = [joined(0, 0, x, z) for x in ahead[2] for z in ahead[3]]

    def device_at(o):
        return rows_ahead[o // (SIDE * SIDE)] + cols_ahead[o % (SIDE * SIDE)]

    loads = []

    def load(src, dst):
        cp = pltpu.make_async_copy(src, dst, load_sem.at[len(loads)])
        cp.start()
        loads.append(cp)

    def factor_at(r, c, size):
        return factor_hbm.at[pl.ds(r * size, size), pl.ds(c * size, size)]

    load(target_hbm, target_ref)
    for t in range(n_tile):
        load(factor_at(2 * t, 2 * t, 128), diag.at[t, 0])
        load(factor_at(2 * t + 1, 2 * t + 1, 128), diag.at[t, 1])
    for t in range(n_tile):
        load(factor_at(2 * t + 1, 2 * t, 128), diag.at[t, 2])
    for t in range(n_big):
        load(factor_at(2 * t + 1, 2 * t, TILE), sub.at[t])
    for p, (i, j) in enumerate(pairs):
        load(factor_at(i, j, BIG), off.at[p])
    load(panel_hbm, panel)
    load(rows_hbm, rows)

    with jax.named_scope("greet"):
        barrier = pltpu.get_barrier_semaphore()
        for o in offsets:
            pl.semaphore_signal(barrier, inc=1, device_id=device_at(o), device_id_type=LOGICAL)

    first, second = 2 * n_tile + 1, 3 * n_tile + n_big + 1
    for cp in loads[:first]:
        cp.wait()
    with jax.named_scope("place"):
        sent = target_ref.shape[1]
        target = jnp.broadcast_to(target_ref[...], (8, sent))
        holder = target // owned
        within = target - holder * owned
        lane = iota((8, sent), 1)
        rank = jnp.zeros((8, sent), I32)
        for d in range(1, SLOTS):
            same = (pltpu.roll(holder, d, 1) == holder) & (lane >= d)
            rank = rank + jnp.where(same, 1, 0)
        away = joined(*(lax.rem(h - c + n, n) for h, c, n in zip(parts_of(holder), here, SIZES)))
        position = (away * SLOTS + rank)[:1]
        slots = n_holders * SLOTS
        placed = jnp.where(iota((slots, sent), 0) == position, 1.0, 0.0).astype(BF16)
        place[...] = placed
        described = jnp.concatenate(
            [jnp.broadcast_to(within[:1].astype(F32), (128, sent)), jnp.ones((128, sent), F32)], axis=0
        ).astype(BF16)
        found = mm_nt(placed, described)
        index = found[:, :128] + EMPTY * (1.0 - found[:, 128:])
        index = jnp.where(iota((slots, 128), 1) == iota((slots, 128), 0) % SLOTS, index, 0.0).astype(BF16)
        turn = iota((n_holders, slots), 0)
        turn = turn % n_row * n_col + turn // n_row
        collect = jnp.where(turn == iota((n_holders, slots), 1) // SLOTS, 1.0, 0.0).astype(BF16)
        row_send[...] = mm(collect, index).reshape(n_col, n_row, 128)
    with jax.named_scope("small"):
        small = invert_small(diag, invert_bases(diag))
    for cp in loads[first:second]:
        cp.wait()
    with jax.named_scope("merge"):
        inverse = invert_tiles(diag, small)
        for b in range(n_big):
            left = split(below(sub[b], inverse[2 * b], inverse[2 * b + 1], TILE))
            top, bottom = split(inverse[2 * b]), split(inverse[2 * b + 1])
            for ref, i in ((vh, 0), (vl, 1)):
                ref[b, 0] = top[i]
                ref[b, 1] = left[i]
                ref[b, 2] = bottom[i]
    for cp in loads[second:]:
        cp.wait()
    with jax.named_scope("split"):
        for p in range(len(pairs)):
            oh[p], ol[p] = split(off[p])
    def dispatch(ch):
        for o in offsets:
            pltpu.make_async_remote_copy(
                src_ref=sends[ch].at[o],
                dst_ref=recvs[ch].at[opposite(o)],
                send_sem=send_sem.at[ch],
                recv_sem=recv_sem.at[ch],
                device_id=device_at(o),
                device_id_type=LOGICAL,
            ).start()
        recvs[ch][0] = sends[ch][0]

    others = pl.ds(1, n_holders - 1)

    def arrived(ch):
        pltpu.make_async_copy(sends[ch].at[others], recvs[ch].at[others], recv_sem.at[ch]).wait()

    def left_device(ch):
        pltpu.make_async_copy(sends[ch].at[others], recvs[ch].at[others], send_sem.at[ch]).wait()

    def start(src, dst, o, at):
        pltpu.make_async_remote_copy(
            src_ref=src, dst_ref=dst, send_sem=send_sem.at[at], recv_sem=recv_sem.at[at],
            device_id=device_at(o), device_id_type=LOGICAL,
        ).start()

    col_peers, row_peers = pl.ds(1, n_col - 1), pl.ds(1, n_row - 1)

    def index_to_row():
        for o in range(1, n_col):
            start(row_send.at[o], row_recv.at[opposite(o)], o, n_chunk)
        row_recv[0] = row_send[0]

    def index_to_col():
        pltpu.make_async_copy(row_send.at[col_peers], row_recv.at[col_peers], recv_sem.at[n_chunk]).wait()
        turn = iota((n_holders, n_holders), 0)
        turn = turn % n_col * n_row + turn // n_col
        turned = jnp.where(turn == iota((n_holders, n_holders), 1), 1.0, 0.0).astype(BF16)
        col_send[...] = mm(turned, row_recv[...].reshape(n_holders, 128).astype(BF16)).reshape(n_row, n_col, 128)
        for r in range(1, n_row):
            start(col_send.at[r], col_recv.at[opposite(r * n_col) // n_col], r * n_col, n_chunk + 1)
        col_recv[0] = col_send[0]

    def index_done():
        pltpu.make_async_copy(row_send.at[col_peers], row_recv.at[col_peers], send_sem.at[n_chunk]).wait()
        for sem in (recv_sem, send_sem):
            pltpu.make_async_copy(col_send.at[row_peers], col_recv.at[row_peers], sem.at[n_chunk + 1]).wait()

    def inv(b, part):
        return (vh[b, part], vl[b, part])

    def halves(x, axis):
        if axis == 0:
            return [tuple(y[:TILE] for y in x), tuple(y[TILE:] for y in x)]
        return [tuple(y[:, :TILE] for y in x), tuple(y[:, TILE:] for y in x)]

    n_chunk = len(sends)
    for ch, (chunk, at0, width) in enumerate(PIECES):
        with jax.named_scope("fwd"):
            if at0 == 0:
                cols = slice(chunk * CHUNK, (chunk + 1) * CHUNK)
                rhs = [panel[b * BIG : (b + 1) * BIG, cols].astype(F32) for b in range(n_big)]
                for b in range(n_big):
                    r = halves(split(rhs[b]), 0)
                    upper = mm3(inv(b, 0), r[0])
                    lower = mm3(inv(b, 2), r[1]) - mm3(inv(b, 1), r[0])
                    f = jnp.concatenate([upper, lower], axis=0)
                    fwd[:, b * BIG : (b + 1) * BIG] = f.T
                    fs = halves(split(f), 0)
                    for p, (i, j) in enumerate(pairs):
                        if j == b:
                            o = halves((oh[p], ol[p]), 1)
                            rhs[i] = (rhs[i] - mm3(o[0], fs[0])) - mm3(o[1], fs[1])
        if ch == 0:
            with jax.named_scope("idx"):
                pl.semaphore_wait(barrier, n_holders - 1)
                index_to_row()
        with jax.named_scope("bwd"):
            mine = slice(at0, at0 + width)
            partial = []
            for b in reversed(range(n_big)):
                q = halves(split(fwd[mine, b * BIG : (b + 1) * BIG]), 1)
                first = mm3(q[0], inv(b, 0)) - mm3(q[1], inv(b, 1))
                second = mm3(q[1], inv(b, 2))
                x = jnp.concatenate([first, second], axis=1)
                xs = halves(split(x), 1)
                for p, (i, j) in reversed(list(enumerate(pairs))):
                    if i == b:
                        at = slice(j * BIG, (j + 1) * BIG)
                        o = halves((oh[p], ol[p]), 0)
                        fwd[mine, at] = (fwd[mine, at] - mm3(xs[0], o[0])) - mm3(xs[1], o[1])
                at = b * BIG
                if b:
                    partial.append(mm_nt(rows[:, at : at + BIG], jnp.concatenate([-xs[0][0], -xs[1][0]], axis=1)))
                else:
                    update = mm_nt(rows[:, :TILE], xs[0][0]) - mm_nt(rows[:, TILE:BIG], -xs[1][0])
            for other in partial:
                update = update - other
            update = update.astype(BF16)
        with jax.named_scope("pack"):
            step = n_holders // GROUPS
            for g in range(GROUPS):
                some = slice(g * step, (g + 1) * step)
                packed = mm(place[g * step * SLOTS : (g + 1) * step * SLOTS], update).reshape(step, SLOTS, width)
                packed = jnp.concatenate([packed[:, :, c : c + 128] for c in range(0, width, 128)], axis=1)
                sends[ch][some] = packed.astype(BF16)
        with jax.named_scope("send"):
            if ch == 1:
                index_to_col()
            dispatch(ch)

    stores = []
    for ch in range(n_chunk):
        with jax.named_scope("wait"):
            arrived(ch)
        with jax.named_scope("final"):
            if ch == 0:
                index_done()
                names = col_recv[...].reshape(n_holders, 128).astype(BF16)
                lanes = jnp.where(iota((128, slots), 0) == iota((128, slots), 1) % SLOTS, 1.0, 0.0).astype(BF16)
                mine = iota((n_holders, slots), 0) == iota((n_holders, slots), 1) // SLOTS
                named = jnp.sum(jnp.where(mine, mm(names, lanes), 0.0), axis=0, keepdims=True)
                gather = jnp.where(iota((owned, slots), 0).astype(F32) == named, 1.0, 0.0).astype(BF16)
            chunk, at0, width = PIECES[ch]
            got = recvs[ch][...].astype(F32)
            got = jnp.concatenate(
                [got[:, c : c + SLOTS].reshape(slots, 128) for c in range(0, width // 128 * SLOTS, SLOTS)], axis=1
            )
            cols = pl.ds(chunk * CHUNK + at0, width)
            result[:, cols] = mm(gather, got.astype(BF16))
        store = pltpu.make_async_copy(result.at[:, cols], out_ref.at[:, cols], load_sem.at[ch])
        store.start()
        stores.append(store)
    for ch in range(n_chunk):
        left_device(ch)
        stores[ch].wait()


def local(coupling_panel, interior_factor, border_rows, target_rows, border_block):
    panel, factor, rows = coupling_panel[0], interior_factor[0], border_rows[0]
    n, width = panel.shape
    holders = lax.axis_size("row") * lax.axis_size("col")
    n_col = lax.axis_size("col")
    n_tile, n_big = n // TILE, n // BIG
    pairs = n_big * (n_big - 1) // 2
    hbm = pl.BlockSpec(memory_space=pl.ANY)
    assembled = pl.pallas_call(
        kernel,
        out_shape=jax.ShapeDtypeStruct(border_block.shape, F32),
        in_specs=[hbm] * 4,
        out_specs=hbm,
        scratch_shapes=[
            pltpu.VMEM(panel.shape, BF16),
            pltpu.VMEM(rows.shape, BF16),
            pltpu.VMEM((n_tile, 3, 128, 128), F32),
            pltpu.VMEM((n_big, TILE, TILE), F32),
            pltpu.VMEM((pairs, BIG, BIG), F32),
            pltpu.VMEM((n_big, 3, TILE, TILE), BF16),
            pltpu.VMEM((n_big, 3, TILE, TILE), BF16),
            pltpu.VMEM((pairs, BIG, BIG), BF16),
            pltpu.VMEM((pairs, BIG, BIG), BF16),
            pltpu.VMEM((CHUNK, n), F32),
            pltpu.VMEM((holders * SLOTS, target_rows.shape[1]), BF16),
            *[pltpu.VMEM((holders, w // 128 * SLOTS, 128), BF16) for _, _, w in PIECES for _ in range(2)],
            pltpu.VMEM((n_col, holders // n_col, 128), F32),
            pltpu.VMEM((n_col, holders // n_col, 128), F32),
            pltpu.VMEM((holders // n_col, n_col, 128), F32),
            pltpu.VMEM((holders // n_col, n_col, 128), F32),
            pltpu.VMEM(target_rows.shape, I32),
            pltpu.VMEM(border_block.shape, F32),
            pltpu.SemaphoreType.DMA((3 * n_tile + n_big + pairs + 3,)),
            pltpu.SemaphoreType.DMA((len(PIECES) + 2,)),
            pltpu.SemaphoreType.DMA((len(PIECES) + 2,)),
        ],
        compiler_params=pltpu.CompilerParams(
            collective_id=0, has_side_effects=True, vmem_limit_bytes=53 * 1024 * 1024
        ),
        name="schur_panel",
    )(panel, factor, rows, target_rows)
    return border_block - assembled


def solution(mesh):
    placed = (
        P("row", None, None),
        P("row", None, None),
        P("row", "col", None),
        P("row", "col"),
        P(("row", "col"), None),
    )
    return jax.shard_map(
        local, mesh=mesh, in_specs=placed, out_specs=P(("row", "col"), None), check_vma=False
    )
```
